16 devices in a mesh: data: 4 (over z, y), sp: 4 (over x, core).
Axes of the slice: x: 2, y: 2, z: 2, core: 2. Of those that a mesh axis runs over, the one named last changes fastest.
Arguments:
- latents: bfloat16 [4, 16, 256, 384], P('data', 'sp'), parts along dimension 0
- norms: float32 [4, 4, 384], replicated
- w_qkv: bfloat16 [4, 384, 3, 6, 64], replicated
- w_out: bfloat16 [4, 6, 64, 384], replicated
- w_up: bfloat16 [4, 384, 1536], replicated
- w_down: bfloat16 [4, 1536, 384], replicated
Outputs:
- output: bfloat16 [4, 16, 256, 384], P('data', None, 'sp'), parts along dimension 0
There are 4 independent parts. The reference program is written for one: setup_inputs(seed, part) draws one part's arguments, and reference() takes and returns one part's arrays. A program takes and returns all parts, laid end to end along the dimension named above; an argument that names none is the same for every part.
All inputs are finite; a program needn't handle non-finite values.
Results may differ from the reference program's by a relative error of at most 0.0159482.
Values are sent between devices in bfloat16 or wider.
A program may use at most 1 GiB of HBM per device.

```python
import math
import jax
import jax.numpy as jnp
from jax import lax

BATCH = 1
FRAMES = 16
PATCHES = 256
WIDTH = 384
HEADS = 6
BLOCKS = 4
HEAD_DIM = WIDTH // HEADS
HIDDEN = 4 * WIDTH
EPS = 1e-6
SPATIAL = (2, 'btqhe,btkhe->bthqk', 'bthqk,btkhe->btqhe')
TEMPORAL = (1, 'bqshe,bkshe->bshqk', 'bshqk,bkshe->bqshe')


def setup_inputs(seed: int = 0, part: int = 0) -> dict:
    base_key = jax.random.key(seed)
    part_key = jax.random.fold_in(base_key, part)
    time_key, space_key, noise_key = jax.random.split(part_key, 3)
    time_walk = jnp.cumsum(jax.random.normal(time_key, (BATCH, FRAMES, WIDTH), jnp.float32), axis=1) * (1.5 / math.sqrt(FRAMES))
    space_walk = jnp.cumsum(jax.random.normal(space_key, (BATCH, PATCHES, WIDTH), jnp.float32), axis=1) * (1.0 / math.sqrt(PATCHES))
    noise = jax.random.normal(noise_key, (BATCH, FRAMES, PATCHES, WIDTH), jnp.float32)
    latents = (time_walk[:, :, None, :] + space_walk[:, None, :, :] + 0.5 * noise).astype(jnp.bfloat16)
    weight_keys = jax.random.split(jax.random.key(seed + 1), 5)
    norm_base = jnp.array([1.0, 0.0, 1.0, 0.0], jnp.float32)
    norms = norm_base[None, :, None] + 0.3 * jax.random.normal(weight_keys[0], (BLOCKS, 4, WIDTH), jnp.float32)
    qkv_gain = jnp.array([1.2, 1.2, 1.0], jnp.float32)[None, None, :, None, None]
    w_qkv = (jax.random.normal(weight_keys[1], (BLOCKS, WIDTH, 3, HEADS, HEAD_DIM), jnp.float32) * qkv_gain / math.sqrt(WIDTH)).astype(jnp.bfloat16)
    w_out = (jax.random.normal(weight_keys[2], (BLOCKS, HEADS, HEAD_DIM, WIDTH), jnp.float32) / math.sqrt(WIDTH)).astype(jnp.bfloat16)
    w_up = (jax.random.normal(weight_keys[3], (BLOCKS, WIDTH, HIDDEN), jnp.float32) / math.sqrt(WIDTH)).astype(jnp.bfloat16)
    w_down = (jax.random.normal(weight_keys[4], (BLOCKS, HIDDEN, WIDTH), jnp.float32) / math.sqrt(HIDDEN)).astype(jnp.bfloat16)
    return {'latents': latents, 'norms': norms, 'w_qkv': w_qkv, 'w_out': w_out, 'w_up': w_up, 'w_down': w_down}


def layer_norm(tokens, norm_gain, norm_shift):
    tokens_f32 = tokens.astype(jnp.float32)
    row_mean = jnp.mean(tokens_f32, axis=-1, keepdims=True)
    centered = tokens_f32 - row_mean
    variance = jnp.mean(jnp.square(centered), axis=-1, keepdims=True)
    return (centered * lax.rsqrt(variance + EPS) * norm_gain + norm_shift).astype(jnp.bfloat16)


def attention(query_rows, key_rows, value_rows, layout):
    seq_axis, score_form, mix_form = layout
    seq_len = query_rows.shape[seq_axis]
    q_block = math.gcd(seq_len, 64)
    logit_scale = HEAD_DIM ** -0.5
    key_f32 = key_rows.astype(jnp.float32)
    value_f32 = value_rows.astype(jnp.float32)

    def attend_block(block_idx, attn_out):
        q_start = block_idx * q_block
        q_part = lax.dynamic_slice_in_dim(query_rows, q_start, q_block, axis=seq_axis).astype(jnp.float32)
        logits = jnp.einsum(score_form, q_part, key_f32) * logit_scale
        attn_probs = jax.nn.softmax(logits, axis=-1).astype(jnp.bfloat16).astype(jnp.float32)
        block_out = jnp.einsum(mix_form, attn_probs, value_f32).astype(jnp.bfloat16)
        return lax.dynamic_update_slice_in_dim(attn_out, block_out, q_start, axis=seq_axis)

    return lax.fori_loop(0, seq_len // q_block, attend_block, jnp.zeros_like(query_rows))


def project_heads(normed, head_weight):
    return jnp.einsum('btsd,dhe->btshe', normed.astype(jnp.float32), head_weight.astype(jnp.float32)).astype(jnp.bfloat16)


def transformer_block(tokens, norm_rows, qkv_weight, out_weight, up_weight, down_weight, layout):
    normed = layer_norm(tokens, norm_rows[0], norm_rows[1])
    mixed_heads = attention(project_heads(normed, qkv_weight[:, 0]), project_heads(normed, qkv_weight[:, 1]), project_heads(normed, qkv_weight[:, 2]), layout)
    attn_proj = jnp.einsum('btshe,hed->btsd', mixed_heads.astype(jnp.float32), out_weight.astype(jnp.float32))
    residual = (tokens.astype(jnp.float32) + attn_proj).astype(jnp.bfloat16)
    normed_mlp = layer_norm(residual, norm_rows[2], norm_rows[3])
    up_proj = jnp.einsum('btsd,df->btsf', normed_mlp.astype(jnp.float32), up_weight.astype(jnp.float32))
    hidden = jax.nn.gelu(up_proj, approximate=True).astype(jnp.bfloat16)
    down_proj = jnp.einsum('btsf,fd->btsd', hidden.astype(jnp.float32), down_weight.astype(jnp.float32))
    return (residual.astype(jnp.float32) + down_proj).astype(jnp.bfloat16)


def reference(latents, norms, w_qkv, w_out, w_up, w_down):
    tokens = latents
    for layer_idx in range(BLOCKS):
        layout = SPATIAL if layer_idx % 2 == 0 else TEMPORAL
        tokens = transformer_block(tokens, norms[layer_idx], w_qkv[layer_idx], w_out[layer_idx], w_up[layer_idx], w_down[layer_idx], layout)
    return tokens
```

```python
import jax
import jax.numpy as jnp
from jax import lax
from jax.experimental import pallas as pl
from jax.experimental.pallas import tpu as pltpu
from jax.sharding import PartitionSpec as P

F32, BF16 = jnp.float32, jnp.bfloat16
EPS = 1e-6
WIDTH, HEAD_DIM, HIDDEN = 384, 64, 1536
NT = (((1,), (1,)), ((), ()))
NN = (((1,), (0,)), ((), ()))
TN = (((0,), (0,)), ((), ()))
SCORE_SCALE = 0.125 * 1.4426950408889634
MESH = pl.DeviceIdType.MESH


def dot(a, b, dims):
    return lax.dot_general(a, b, dims, preferred_element_type=F32)


def layer_norm(x, gain, shift):
    centered = x - jnp.sum(x, -1, keepdims=True) * (1.0 / WIDTH)
    variance = jnp.sum(centered * centered, -1, keepdims=True) * (1.0 / WIDTH)
    return (centered * lax.rsqrt(variance + EPS) * gain + shift).astype(BF16)


def gelu(x):
    c = 0.7978845608028654
    half = 0.5 * x
    return (half + half * jnp.tanh(x * (c + (c * 0.044715) * (x * x)))).astype(BF16)


def softmax_keys(scores, mask=None):
    if mask is not None:
        scores = jnp.where(mask, scores, -jnp.inf)
    peak = jnp.max(scores, 0, keepdims=True)
    e = jnp.exp2((scores - peak) * SCORE_SCALE)
    return (e * (1.0 / jnp.sum(e, 0, keepdims=True))).astype(BF16)


def swap_halves(x, a, b):
    return x.reshape(a, b, 8, WIDTH).transpose(1, 0, 2, 3).reshape(256, WIDTH)


def block(u, l, norms, wq, wo, wu, wd, hid, temporal):
    x = u.astype(F32)
    if temporal:
        x = swap_halves(x, 16, 2)
    a = layer_norm(x, norms[l, 0:1, :], norms[l, 1:2, :])
    qT = dot(wq[l, 0:384, :], a, NT).astype(BF16)
    k = dot(a, wq[l, 384:768, :], NT).astype(BF16)
    vT = dot(wq[l, 768:1152, :], a, NT).astype(BF16)
    outs = []
    if not temporal:
        zero = jnp.zeros((64, 256), BF16)
        for p in range(3):
            kp = k[:, 128 * p:128 * p + 128]
            for j in range(2):
                h = 64 * (2 * p + j)
                qh = qT[h:h + 64, :]
                rhs = jnp.concatenate([qh, zero] if j == 0 else [zero, qh], 0)
                pT = softmax_keys(dot(kp, rhs, NN))
                outs.append(dot(vT[h:h + 64, :], pT, NN).astype(BF16))
    else:
        zero = jnp.zeros((64, 128), BF16)
        row = lax.broadcasted_iota(jnp.int32, (128, 256), 0)
        col = lax.broadcasted_iota(jnp.int32, (128, 256), 1)
        mask = (row & 7) == (col & 7)
        for p in range(3):
            h = 128 * p
            even, odd = [], []
            for i in range(2):
                t = 128 * i
                q0 = jnp.concatenate([qT[h:h + 64, t:t + 128], zero], 1)
                q1 = jnp.concatenate([zero, qT[h + 64:h + 128, t:t + 128]], 1)
                scores = dot(k[t:t + 128, h:h + 128], jnp.concatenate([q0, q1], 0), NN)
                pT = softmax_keys(scores, mask)
                o = dot(vT[h:h + 128, t:t + 128], pT, NN).astype(BF16)
                even.append(o[0:64, 0:128])
                odd.append(o[64:128, 128:256])
            outs += [jnp.concatenate(even, 1), jnp.concatenate(odd, 1)]
    oT = jnp.concatenate(outs, 0)
    res = (x + dot(oT, wo[l], TN)).astype(BF16).astype(F32)
    a2 = layer_norm(res, norms[l, 2:3, :], norms[l, 3:4, :])
    for c in range(0, HIDDEN, 512):
        hid[:, c:c + 512] = gelu(dot(a2, wu[l, :, c:c + 512], NN))
    z = res + dot(hid[...], wd[l], NN)
    if temporal:
        z = swap_halves(z, 2, 16)
    return z.astype(BF16)


def kernel(x_hbm, norms, wq_hbm, wo_hbm, wu_hbm, wd_hbm, y_hbm,
           xb, wq, wo, wu, wd, hid, frames0, frames1, frames2, cols0, cols1, cols2,
           load_sem, send_sem, recv_sem):
    me = lax.axis_index('sp')
    loads = []
    for l in range(4):
        pairs = ((wq_hbm, wq), (wo_hbm, wo), (wu_hbm, wu), (wd_hbm, wd))
        loads.append([pltpu.make_async_copy(s.at[l], d.at[l], load_sem.at[l, i]) for i, (s, d) in enumerate(pairs)])
    x_load = pltpu.make_async_copy(x_hbm, xb, load_sem.at[4, 0])
    x_load.start()
    for group in loads:
        for c in group:
            c.start()
    barrier = pltpu.get_barrier_semaphore()
    for d in range(1, 4):
        pl.semaphore_signal(barrier, inc=1, device_id={'sp': (me + d) % 4}, device_id_type=MESH)
    pl.semaphore_wait(barrier, 3)
    x_load.wait()

    def to_columns(e, src, dst, f, d):
        peer = (me + d) % 4
        rows = pl.ds(pl.multiple_of(64 * peer, 64), 64)
        return pltpu.make_async_remote_copy(
            src_ref=src.at[f, rows, :], dst_ref=dst.at[4 * me + f],
            send_sem=send_sem.at[e, f, d - 1], recv_sem=recv_sem.at[e, f, d - 1],
            device_id={'sp': peer}, device_id_type=MESH)

    def to_frames(e, src, dst, g, d):
        peer = (me + d) % 4
        return pltpu.make_async_remote_copy(
            src_ref=src.at[pl.ds(4 * peer, 4), pl.ds(pl.multiple_of(16 * g, 16), 16), :],
            dst_ref=dst.at[:, pl.ds(pl.multiple_of(64 * me + 16 * g, 16), 16), :],
            send_sem=send_sem.at[e, g, d - 1], recv_sem=recv_sem.at[e, g, d - 1],
            device_id={'sp': peer}, device_id_type=MESH)

    def spatial(l, e, src, out, dst):
        def body(f, _):
            z = block(src[f], l, norms, wq, wo, wu, wd, hid, False)
            out[f] = z
            for d in range(1, 4):
                to_columns(e, out, dst, f, d).start()
            dst[4 * me + f] = out[f, pl.ds(pl.multiple_of(64 * me, 64), 64), :]
            return 0
        lax.fori_loop(0, 4, body, 0)

    def wait_all(e, make, src, dst):
        for f in range(4):
            for d in range(1, 4):
                c = make(e, src, dst, f, d)
                c.wait_recv()
                c.wait_send()

    def temporal(l, e, src, out, dst):
        def body(g, _):
            cols = pl.ds(pl.multiple_of(16 * g, 16), 16)
            z = block(src[:, cols, :].reshape(256, WIDTH), l, norms, wq, wo, wu, wd, hid, True)
            out[:, cols, :] = z.reshape(16, 16, WIDTH)
            if dst is not None:
                for d in range(1, 4):
                    to_frames(e, out, dst, g, d).start()
                mine = pl.ds(pl.multiple_of(64 * me + 16 * g, 16), 16)
                dst[:, mine, :] = out[pl.ds(4 * me, 4), cols, :]
            return 0
        lax.fori_loop(0, 4, body, 0)

    def wait_weights(l):
        for c in loads[l]:
            c.wait()

    wait_weights(0)
    spatial(0, 0, xb, frames0, cols0)
    wait_weights(1)
    wait_all(0, to_columns, frames0, cols0)
    temporal(1, 1, cols0, cols1, frames1)
    wait_weights(2)
    wait_all(1, to_frames, cols1, frames1)
    spatial(2, 2, frames1, frames2, cols2)
    wait_weights(3)
    wait_all(2, to_columns, frames2, cols2)
    temporal(3, 3, cols2, cols0, None)
    y_store = pltpu.make_async_copy(cols0, y_hbm, load_sem.at[4, 1])
    y_store.start()
    y_store.wait()


def solution(mesh):
    anyspace = pl.BlockSpec(memory_space=pl.ANY)

    def local_stack(latents, norms, w_qkv, w_out, w_up, w_down):
        frames = (4, 256, WIDTH)
        cols = (16, 64, WIDTH)
        out = pl.pallas_call(
            kernel,
            out_shape=jax.ShapeDtypeStruct(cols, BF16),
            in_specs=[anyspace, pl.BlockSpec(memory_space=pltpu.VMEM)] + [anyspace] * 4,
            out_specs=anyspace,
            scratch_shapes=[
                pltpu.VMEM(frames, BF16),
                pltpu.VMEM((4, 1152, WIDTH), BF16), pltpu.VMEM((4, WIDTH, WIDTH), BF16),
                pltpu.VMEM((4, WIDTH, HIDDEN), BF16), pltpu.VMEM((4, HIDDEN, WIDTH), BF16),
                pltpu.VMEM((256, HIDDEN), BF16),
                pltpu.VMEM(frames, BF16), pltpu.VMEM(frames, BF16), pltpu.VMEM(frames, BF16),
                pltpu.VMEM(cols, BF16), pltpu.VMEM(cols, BF16), pltpu.VMEM(cols, BF16),
                pltpu.SemaphoreType.DMA((5, 4)),
                pltpu.SemaphoreType.DMA((3, 4, 3)),
                pltpu.SemaphoreType.DMA((3, 4, 3)),
            ],
            compiler_params=pltpu.CompilerParams(collective_id=0, has_side_effects=True, vmem_limit_bytes=56 * 2**20),
        )(latents[0], norms,
          w_qkv.transpose(0, 2, 3, 4, 1).reshape(4, 3 * WIDTH, WIDTH),
          w_out.reshape(4, WIDTH, WIDTH), w_up, w_down)
        return out[None]

    whole = P()
    return jax.shard_map(local_stack, mesh=mesh,
                         in_specs=(P('data', 'sp', None, None), whole, whole, whole, whole, whole),
                         out_specs=P('data', None, 'sp', None), check_vma=False)
```

```python
import jax
import jax.numpy as jnp
from jax import lax
from jax.experimental import pallas as pl
from jax.experimental.pallas import tpu as pltpu
from jax.sharding import PartitionSpec as P

F32, BF16 = jnp.float32, jnp.bfloat16
EPS = 1e-6
WIDTH, HEAD_DIM, HIDDEN = 384, 64, 1536
NT = (((1,), (1,)), ((), ()))
NN = (((1,), (0,)), ((), ()))
TN = (((0,), (0,)), ((), ()))
SCORE_SCALE = 0.125 * 1.4426950408889634
MESH = pl.DeviceIdType.MESH


def dot(a, b, dims):
    return lax.dot_general(a, b, dims, preferred_element_type=F32)


def layer_norm(x, gain, shift):
    centered = x - jnp.sum(x, -1, keepdims=True) * (1.0 / WIDTH)
    variance = jnp.sum(centered * centered, -1, keepdims=True) * (1.0 / WIDTH)
    return (centered * lax.rsqrt(variance + EPS) * gain + shift).astype(BF16)


def gelu(x):
    c = 0.7978845608028654
    half = 0.5 * x
    return (half + half * jnp.tanh(x * (c + (c * 0.044715) * (x * x)))).astype(BF16)


def swap_halves(x, a, b):
    return x.reshape(a, b, 8, WIDTH).transpose(1, 0, 2, 3).reshape(256, WIDTH)


def block(u, l, norms, wq, wo, wu, wd, hid, scratch, temporal):
    x = u.astype(F32)
    if temporal:
        x = swap_halves(x, 16, 2)
    a = layer_norm(x, norms[l, 0:1, :], norms[l, 1:2, :])
    qT = dot(wq[l, 0:384, :], a, NT).astype(BF16)
    k = dot(a, wq[l, 384:768, :], NT).astype(BF16)
    vT = dot(wq[l, 768:1152, :], a, NT).astype(BF16)
    scores, expd, probs, mixed = scratch
    if not temporal:
        zero = jnp.zeros((64, 256), BF16)
        for h in range(6):
            qh = qT[64 * h:64 * h + 64, :]
            rhs = jnp.concatenate([zero, qh] if h % 2 else [qh, zero], 0)
            p = h // 2 * 128
            scores[h] = dot(k[:, p:p + 128], rhs, NN)
    else:
        zero = jnp.zeros((64, 128), BF16)
        row = lax.broadcasted_iota(jnp.int32, (128, 256), 0)
        col = lax.broadcasted_iota(jnp.int32, (128, 256), 1)
        same_patch = (row & 7) == (col & 7)
        for h in range(6):
            p, t = h // 2 * 128, h % 2 * 128
            q0 = jnp.concatenate([qT[p:p + 64, t:t + 128], zero], 1)
            q1 = jnp.concatenate([zero, qT[p + 64:p + 128, t:t + 128]], 1)
            s = dot(k[t:t + 128, p:p + 128], jnp.concatenate([q0, q1], 0), NN)
            scores[h, 0:128] = jnp.where(same_patch, s, -jnp.inf)
    keys = 128 if temporal else 256
    for h in range(6):
        peak = jnp.max(scores[h, 0:keys], 0, keepdims=True)
        e = jnp.exp2((scores[h, 0:keys] - peak) * SCORE_SCALE)
        expd[h, 0:keys] = e
        inverse = 1.0 / jnp.sum(e, 0, keepdims=True)
        probs[h, 0:keys] = (expd[h, 0:keys] * inverse).astype(BF16)
    for h in range(6):
        if not temporal:
            r = 64 * h
            mixed[r:r + 64, :] = dot(vT[r:r + 64, :], probs[h], NN).astype(BF16)
        else:
            p, t = h // 2 * 128, h % 2 * 128
            o = dot(vT[p:p + 128, t:t + 128], probs[h, 0:128], NN).astype(BF16)
            mixed[p:p + 64, t:t + 128] = o[0:64, 0:128]
            mixed[p + 64:p + 128, t:t + 128] = o[64:128, 128:256]
    oT = mixed[...]
    res = (x + dot(oT, wo[l], TN)).astype(BF16).astype(F32)
    a2 = layer_norm(res, norms[l, 2:3, :], norms[l, 3:4, :])
    for c in range(0, HIDDEN, 512):
        hid[:, c:c + 512] = gelu(dot(a2, wu[l, :, c:c + 512], NN))
    z = res + dot(hid[...], wd[l], NN)
    if temporal:
        z = swap_halves(z, 2, 16)
    return z.astype(BF16)


def kernel(x_hbm, norms, wq_hbm, wo_hbm, wu_hbm, wd_hbm, y_hbm,
           xb, wq, wo, wu, wd, hid, frames0, frames1, frames2, cols0, cols1, cols2,
           load_sem, send_sem, recv_sem, *scratch):
    me = lax.axis_index('sp')
    loads = []
    for l in range(4):
        pairs = ((wq_hbm, wq), (wo_hbm, wo), (wu_hbm, wu), (wd_hbm, wd))
        loads.append([pltpu.make_async_copy(s.at[l], d.at[l], load_sem.at[l, i]) for i, (s, d) in enumerate(pairs)])
    x_load = pltpu.make_async_copy(x_hbm, xb, load_sem.at[4, 0])
    x_load.start()
    for c in loads[0]:
        c.start()
    barrier = pltpu.get_barrier_semaphore()
    for d in range(1, 4):
        pl.semaphore_signal(barrier, inc=1, device_id={'sp': (me + d) % 4}, device_id_type=MESH)
    pl.semaphore_wait(barrier, 3)
    x_load.wait()

    def to_columns(e, src, dst, f, d):
        peer = (me + d) % 4
        rows = pl.ds(pl.multiple_of(64 * peer, 64), 64)
        return pltpu.make_async_remote_copy(
            src_ref=src.at[f, rows, :], dst_ref=dst.at[4 * me + f],
            send_sem=send_sem.at[e, f, d - 1], recv_sem=recv_sem.at[e, f, d - 1],
            device_id={'sp': peer}, device_id_type=MESH)

    def to_frames(e, src, dst, g, d):
        peer = (me + d) % 4
        return pltpu.make_async_remote_copy(
            src_ref=src.at[pl.ds(4 * peer, 4), pl.ds(pl.multiple_of(16 * g, 16), 16), :],
            dst_ref=dst.at[:, pl.ds(pl.multiple_of(64 * me + 16 * g, 16), 16), :],
            send_sem=send_sem.at[e, g, d - 1], recv_sem=recv_sem.at[e, g, d - 1],
            device_id={'sp': peer}, device_id_type=MESH)

    def spatial(l, e, src, out, dst):
        def body(f, _):
            z = block(src[f], l, norms, wq, wo, wu, wd, hid, scratch, False)
            out[f] = z
            for d in range(1, 4):
                to_columns(e, out, dst, f, d).start()
            dst[4 * me + f] = out[f, pl.ds(pl.multiple_of(64 * me, 64), 64), :]
            return 0
        lax.fori_loop(0, 4, body, 0)

    def wait_all(e, make, src, dst):
        for f in range(4):
            for d in range(1, 4):
                c = make(e, src, dst, f, d)
                c.wait_recv()
                c.wait_send()

    def temporal(l, e, src, out, dst):
        def body(g, _):
            cols = pl.ds(pl.multiple_of(16 * g, 16), 16)
            z = block(src[:, cols, :].reshape(256, WIDTH), l, norms, wq, wo, wu, wd, hid, scratch, True)
            out[:, cols, :] = z.reshape(16, 16, WIDTH)
            if dst is not None:
                for d in range(1, 4):
                    to_frames(e, out, dst, g, d).start()
                mine = pl.ds(pl.multiple_of(64 * me + 16 * g, 16), 16)
                dst[:, mine, :] = out[pl.ds(4 * me, 4), cols, :]
            return 0
        lax.fori_loop(0, 4, body, 0)

    def wait_weights(l):
        for c in loads[l]:
            c.wait()

    wait_weights(0)
    for group in loads[1:]:
        for c in group:
            c.start()
    spatial(0, 0, xb, frames0, cols0)
    wait_weights(1)
    wait_all(0, to_columns, frames0, cols0)
    temporal(1, 1, cols0, cols1, frames1)
    wait_weights(2)
    wait_all(1, to_frames, cols1, frames1)
    spatial(2, 2, frames1, frames2, cols2)
    wait_weights(3)
    wait_all(2, to_columns, frames2, cols2)
    temporal(3, 3, cols2, cols0, None)
    y_store = pltpu.make_async_copy(cols0, y_hbm, load_sem.at[4, 1])
    y_store.start()
    y_store.wait()


def solution(mesh):
    anyspace = pl.BlockSpec(memory_space=pl.ANY)

    def local_stack(latents, norms, w_qkv, w_out, w_up, w_down):
        frames = (4, 256, WIDTH)
        cols = (16, 64, WIDTH)
        out = pl.pallas_call(
            kernel,
            out_shape=jax.ShapeDtypeStruct(cols, BF16),
            in_specs=[anyspace, pl.BlockSpec(memory_space=pltpu.VMEM)] + [anyspace] * 4,
            out_specs=anyspace,
            scratch_shapes=[
                pltpu.VMEM(frames, BF16),
                pltpu.VMEM((4, 1152, WIDTH), BF16), pltpu.VMEM((4, WIDTH, WIDTH), BF16),
                pltpu.VMEM((4, WIDTH, HIDDEN), BF16), pltpu.VMEM((4, HIDDEN, WIDTH), BF16),
                pltpu.VMEM((256, HIDDEN), BF16),
                pltpu.VMEM(frames, BF16), pltpu.VMEM(frames, BF16), pltpu.VMEM(frames, BF16),
                pltpu.VMEM(cols, BF16), pltpu.VMEM(cols, BF16), pltpu.VMEM(cols, BF16),
                pltpu.SemaphoreType.DMA((5, 4)),
                pltpu.SemaphoreType.DMA((3, 4, 3)),
                pltpu.SemaphoreType.DMA((3, 4, 3)),
                pltpu.VMEM((6, 256, 256), F32), pltpu.VMEM((6, 256, 256), F32),
                pltpu.VMEM((6, 256, 256), BF16), pltpu.VMEM((WIDTH, 256), BF16),
            ],
            compiler_params=pltpu.CompilerParams(collective_id=0, has_side_effects=True, vmem_limit_bytes=56 * 2**20),
        )(latents[0], norms,
          w_qkv.transpose(0, 2, 3, 4, 1).reshape(4, 3 * WIDTH, WIDTH),
          w_out.reshape(4, WIDTH, WIDTH), w_up, w_down)
        return out[None]

    whole = P()
    return jax.shard_map(local_stack, mesh=mesh,
                         in_specs=(P('data', 'sp', None, None), whole, whole, whole, whole, whole),
                         out_specs=P('data', None, 'sp', None), check_vma=False)
```

```python
import jax
import jax.numpy as jnp
from jax import lax
from jax.experimental import pallas as pl
from jax.experimental.pallas import tpu as pltpu
from jax.sharding import PartitionSpec as P

F32, BF16 = jnp.float32, jnp.bfloat16
EPS = 1e-6
WIDTH, HIDDEN = 384, 1536
NT = (((1,), (1,)), ((), ()))
NN = (((1,), (0,)), ((), ()))
TN = (((0,), (0,)), ((), ()))
SCORE_SCALE = 0.125 * 1.4426950408889634
MESH = pl.DeviceIdType.MESH


def dot(a, b, dims):
    return lax.dot_general(a, b, dims, preferred_element_type=F32)


def layer_norm(x, gain, shift):
    centered = x - jnp.sum(x, -1, keepdims=True) * (1.0 / WIDTH)
    variance = jnp.sum(centered * centered, -1, keepdims=True) * (1.0 / WIDTH)
    return (centered * lax.rsqrt(variance + EPS) * gain + shift).astype(BF16)


def gelu(x):
    c = 0.7978845608028654
    half = 0.5 * x
    return (half + half * jnp.tanh(x * (c + (c * 0.044715) * (x * x)))).astype(BF16)


def swap_halves(x, a, b):
    return x.reshape(a, b, 8, WIDTH).transpose(1, 0, 2, 3).reshape(256, WIDTH)


def head_scores(qT, k, scores, temporal):
    if not temporal:
        zero = jnp.zeros((64, 256), BF16)
        for h in range(6):
            qh = qT[64 * h:64 * h + 64, :]
            rhs = jnp.concatenate([zero, qh] if h % 2 else [qh, zero], 0)
            p = h // 2 * 128
            scores[h] = dot(k[:, p:p + 128], rhs, NN)
    else:
        zero = jnp.zeros((64, 128), BF16)
        row = lax.broadcasted_iota(jnp.int32, (128, 256), 0)
        col = lax.broadcasted_iota(jnp.int32, (128, 256), 1)
        same_patch = (row & 7) == (col & 7)
        for h in range(6):
            p, t = h // 2 * 128, h % 2 * 128
            q0 = jnp.concatenate([qT[p:p + 64, t:t + 128], zero], 1)
            q1 = jnp.concatenate([zero, qT[p + 64:p + 128, t:t + 128]], 1)
            s = dot(k[t:t + 128, p:p + 128], jnp.concatenate([q0, q1], 0), NN)
            scores[h, 0:128] = jnp.where(same_patch, s, -jnp.inf)


def head_probs(scores, expd, probs, temporal):
    keys = 128 if temporal else 256
    for h in range(6):
        peak = jnp.max(scores[h, 0:keys], 0, keepdims=True)
        e = jnp.exp2((scores[h, 0:keys] - peak) * SCORE_SCALE)
        expd[h, 0:keys] = e
        inverse = 1.0 / jnp.sum(e, 0, keepdims=True)
        probs[h, 0:keys] = (expd[h, 0:keys] * inverse).astype(BF16)


def head_mix(vT, probs, mixed, temporal):
    for h in range(6):
        if not temporal:
            r = 64 * h
            mixed[r:r + 64, :] = dot(vT[r:r + 64, :], probs[h], NN).astype(BF16)
        else:
            p, t = h // 2 * 128, h % 2 * 128
            o = dot(vT[p:p + 128, t:t + 128], probs[h, 0:128], NN).astype(BF16)
            mixed[p:p + 64, t:t + 128] = o[0:64, 0:128]
            mixed[p + 64:p + 128, t:t + 128] = o[64:128, 128:256]


def attend(xs, l, norms, wq, wo, scratch, temporal):
    kept = []
    for j, x in enumerate(xs):
        a = layer_norm(x, norms[l, 0:1, :], norms[l, 1:2, :])
        qT = dot(wq[l, 0:384, :], a, NT).astype(BF16)
        k = dot(a, wq[l, 384:768, :], NT).astype(BF16)
        kept.append(dot(wq[l, 768:1152, :], a, NT).astype(BF16))
        head_scores(qT, k, scratch[0].at[j], temporal)
    for j in range(len(xs)):
        head_probs(scratch[0].at[j], scratch[1].at[j], scratch[2].at[j], temporal)
    for j in range(len(xs)):
        head_mix(kept[j], scratch[2].at[j], scratch[3].at[j], temporal)
    return [(x + dot(scratch[3][j], wo[l], TN)).astype(BF16) for j, x in enumerate(xs)]


def mlp(res, l, norms, wu, wd, hid):
    res = res.astype(F32)
    a = layer_norm(res, norms[l, 2:3, :], norms[l, 3:4, :])
    for c in range(0, HIDDEN, 512):
        hid[:, c:c + 512] = gelu(dot(a, wu[l, :, c:c + 512], NN))
    return res + dot(hid[...], wd[l], NN)


def kernel(x_hbm, norms, wq_hbm, wo_hbm, wu_hbm, wd_hbm, y_hbm,
           xb, wq, wo, wu, wd, hid, res, sent0, cols1, sent1, frames2, sent2, cols3, yb,
           load_sem, send_sem, recv_sem, *scratch):
    me = lax.axis_index('sp')
    pairs = ((wq_hbm, wq), (wo_hbm, wo), (wu_hbm, wu), (wd_hbm, wd))
    loads = [[pltpu.make_async_copy(s.at[l], d.at[l], load_sem.at[l, i]) for i, (s, d) in enumerate(pairs)]
             for l in range(4)]
    x_load = pltpu.make_async_copy(x_hbm, xb, load_sem.at[4, 0])
    x_load.start()
    for c in loads[0]:
        c.start()
    barrier = pltpu.get_barrier_semaphore()
    for d in range(1, 4):
        pl.semaphore_signal(barrier, inc=1, device_id={'sp': (me + d) % 4}, device_id_type=MESH)
    pl.semaphore_wait(barrier, 3)

    def to_columns(e, src, dst, g, d):
        peer = (me + d) % 4
        return pltpu.make_async_remote_copy(
            src_ref=src.at[g, peer], dst_ref=dst.at[g, pl.ds(4 * me, 4)],
            send_sem=send_sem.at[e, g, d - 1], recv_sem=recv_sem.at[e, g, d - 1],
            device_id={'sp': peer}, device_id_type=MESH)

    def to_frames(e, src, dst, g, d):
        peer = (me + d) % 4
        return pltpu.make_async_remote_copy(
            src_ref=src.at[g, pl.ds(4 * peer, 4)], dst_ref=dst.at[me, g],
            send_sem=send_sem.at[e, g, d - 1], recv_sem=recv_sem.at[e, g, d - 1],
            device_id={'sp': peer}, device_id_type=MESH)

    def spatial(l, e, read_frame, sent, dst):
        def attention_pair(i, _):
            rows = attend([read_frame(2 * i + j).astype(F32) for j in range(2)], l, norms, wq, wo, scratch, False)
            for j in range(2):
                res[2 * i + j] = rows[j].reshape(4, 4, 16, WIDTH)
            return 0

        def mlp_group(g, _):
            rows = jnp.stack([res[:, j, g] for j in range(4)])
            z = mlp(rows.reshape(256, WIDTH), l, norms, wu, wd, hid)
            sent[g] = z.astype(BF16).reshape(4, 4, 16, WIDTH)
            for d in (2, 1, 3):
                to_columns(e, sent, dst, g, d).start()
            dst[g, pl.ds(4 * me, 4)] = sent[g, me]
            return 0

        lax.fori_loop(0, 2, attention_pair, 0)
        lax.fori_loop(0, 4, mlp_group, 0)

    def temporal(l, e, src, write):
        def body(g, _):
            for d in (1, 2, 3):
                to_columns(e, sent0, src, g, d).wait_recv()
            x = swap_halves(src[g].reshape(256, WIDTH).astype(F32), 16, 2)
            rows = attend([x], l, norms, wq, wo, scratch, True)
            z = mlp(rows[0], l, norms, wu, wd, hid)
            write(g, swap_halves(z, 2, 16).astype(BF16).reshape(16, 16, WIDTH))
            return 0
        lax.fori_loop(0, 4, body, 0)

    def send_to_frames(g, z):
        sent1[g] = z
        for d in (2, 1, 3):
            to_frames(1, sent1, frames2, g, d).start()
        frames2[me, g] = sent1[g, pl.ds(4 * me, 4)]

    def y_store(g):
        return pltpu.make_async_copy(yb.at[g], y_hbm.at[:, pl.ds(pl.multiple_of(16 * g, 16), 16), :],
                                     load_sem.at[5, g])

    def write_y(g, z):
        yb[g] = z
        y_store(g).start()

    def wait_weights(l):
        for c in loads[l]:
            c.wait()

    x_load.wait()
    wait_weights(0)
    for group in loads[1:]:
        for c in group:
            c.start()
    spatial(0, 0, lambda f: xb[f], sent0, cols1)
    wait_weights(1)
    temporal(1, 0, cols1, send_to_frames)
    wait_weights(2)
    for g in range(4):
        for d in (1, 2, 3):
            to_frames(1, sent1, frames2, g, d).wait_recv()
    spatial(2, 2, lambda f: frames2[:, :, f].reshape(256, WIDTH), sent2, cols3)
    wait_weights(3)
    temporal(3, 2, cols3, write_y)
    for g in range(4):
        y_store(g).wait()
        for d in (1, 2, 3):
            to_columns(0, sent0, cols1, g, d).wait_send()
            to_frames(1, sent1, frames2, g, d).wait_send()
            to_columns(2, sent2, cols3, g, d).wait_send()


def solution(mesh):
    anyspace = pl.BlockSpec(memory_space=pl.ANY)

    def local_stack(latents, norms, w_qkv, w_out, w_up, w_down):
        tokens = (4, 4, 4, 16, WIDTH)
        groups = (4, 16, 16, WIDTH)
        out = pl.pallas_call(
            kernel,
            out_shape=jax.ShapeDtypeStruct((16, 64, WIDTH), BF16),
            in_specs=[anyspace, pl.BlockSpec(memory_space=pltpu.VMEM)] + [anyspace] * 4,
            out_specs=anyspace,
            scratch_shapes=[
                pltpu.VMEM((4, 256, WIDTH), BF16),
                pltpu.VMEM((4, 1152, WIDTH), BF16), pltpu.VMEM((4, WIDTH, WIDTH), BF16),
                pltpu.VMEM((4, WIDTH, HIDDEN), BF16), pltpu.VMEM((4, HIDDEN, WIDTH), BF16),
                pltpu.VMEM((256, HIDDEN), BF16),
                pltpu.VMEM(tokens, BF16),
                pltpu.VMEM(tokens, BF16), pltpu.VMEM(groups, BF16),
                pltpu.VMEM(groups, BF16), pltpu.VMEM(tokens, BF16),
                pltpu.VMEM(tokens, BF16), pltpu.VMEM(groups, BF16),
                pltpu.VMEM(groups, BF16),
                pltpu.SemaphoreType.DMA((6, 4)),
                pltpu.SemaphoreType.DMA((3, 4, 3)),
                pltpu.SemaphoreType.DMA((3, 4, 3)),
                pltpu.VMEM((2, 6, 256, 256), F32), pltpu.VMEM((2, 6, 256, 256), F32),
                pltpu.VMEM((2, 6, 256, 256), BF16), pltpu.VMEM((2, WIDTH, 256), BF16),
            ],
            compiler_params=pltpu.CompilerParams(collective_id=0, has_side_effects=True, vmem_limit_bytes=56 * 2**20),
        )(latents[0], norms,
          w_qkv.transpose(0, 2, 3, 4, 1).reshape(4, 3 * WIDTH, WIDTH),
          w_out.reshape(4, WIDTH, WIDTH), w_up, w_down)
        return out[None]

    whole = P()
    return jax.shard_map(local_stack, mesh=mesh,
                         in_specs=(P('data', 'sp', None, None), whole, whole, whole, whole, whole),
                         out_specs=P('data', None, 'sp', None), check_vma=False)
```

```python
import jax
import jax.numpy as jnp
from jax import lax
from jax.experimental import pallas as pl
from jax.experimental.pallas import tpu as pltpu
from jax.sharding import PartitionSpec as P

F32, BF16 = jnp.float32, jnp.bfloat16
EPS = 1e-6
WIDTH, HIDDEN = 384, 1536
NT = (((1,), (1,)), ((), ()))
NN = (((1,), (0,)), ((), ()))
TN = (((0,), (0,)), ((), ()))
SCORE_SCALE = 0.125 * 1.4426950408889634
MESH = pl.DeviceIdType.MESH


def dot(a, b, dims):
    return lax.dot_general(a, b, dims, preferred_element_type=F32)


def layer_norm(x, gain, shift):
    centered = x - jnp.sum(x, -1, keepdims=True) * (1.0 / WIDTH)
    variance = jnp.sum(centered * centered, -1, keepdims=True) * (1.0 / WIDTH)
    return (centered * lax.rsqrt(variance + EPS) * gain + shift).astype(BF16)


def gelu(x):
    c = 0.7978845608028654
    half = 0.5 * x
    return (half + half * jnp.tanh(x * (c + (c * 0.044715) * (x * x)))).astype(BF16)


def swap_halves(x, a, b):
    return x.reshape(a, b, 8, WIDTH).transpose(1, 0, 2, 3).reshape(256, WIDTH)


def head_scores(qT, k, scores, temporal):
    if not temporal:
        zero = jnp.zeros((64, 256), BF16)
        for h in range(6):
            qh = qT[64 * h:64 * h + 64, :]
            rhs = jnp.concatenate([zero, qh] if h % 2 else [qh, zero], 0)
            p = h // 2 * 128
            scores[h] = dot(k[:, p:p + 128], rhs, NN)
    else:
        zero = jnp.zeros((64, 128), BF16)
        row = lax.broadcasted_iota(jnp.int32, (128, 256), 0)
        col = lax.broadcasted_iota(jnp.int32, (128, 256), 1)
        same_patch = (row & 7) == (col & 7)
        for h in range(6):
            p, t = h // 2 * 128, h % 2 * 128
            q0 = jnp.concatenate([qT[p:p + 64, t:t + 128], zero], 1)
            q1 = jnp.concatenate([zero, qT[p + 64:p + 128, t:t + 128]], 1)
            s = dot(k[t:t + 128, p:p + 128], jnp.concatenate([q0, q1], 0), NN)
            scores[h, 0:128] = jnp.where(same_patch, s, -jnp.inf)


def head_probs(scores, expd, probs, temporal):
    keys = 128 if temporal else 256
    for h in range(6):
        peak = jnp.max(scores[h, 0:keys], 0, keepdims=True)
        e = jnp.exp2((scores[h, 0:keys] - peak) * SCORE_SCALE)
        expd[h, 0:keys] = e
        inverse = 1.0 / jnp.sum(e, 0, keepdims=True)
        probs[h, 0:keys] = (expd[h, 0:keys] * inverse).astype(BF16)


def head_mix(vT, probs, mixed, temporal):
    for h in range(6):
        if not temporal:
            r = 64 * h
            mixed[r:r + 64, :] = dot(vT[r:r + 64, :], probs[h], NN).astype(BF16)
        else:
            p, t = h // 2 * 128, h % 2 * 128
            o = dot(vT[p:p + 128, t:t + 128], probs[h, 0:128], NN).astype(BF16)
            mixed[p:p + 64, t:t + 128] = o[0:64, 0:128]
            mixed[p + 64:p + 128, t:t + 128] = o[64:128, 128:256]


def head_scores_rows(q, k, scores):
    low = lax.broadcasted_iota(jnp.int32, (256, 128), 1) < 64
    for h in range(6):
        p = h // 2 * 128
        qp = q[:, p:p + 128]
        zero = jnp.zeros_like(qp)
        rhs = jnp.where(low, zero, qp) if h % 2 else jnp.where(low, qp, zero)
        scores[h] = dot(k[:, p:p + 128], rhs, NT)


def attend_end(xs, values, l, wo, scratch, temporal):
    for j in range(len(xs)):
        head_probs(scratch[0].at[j], scratch[1].at[j], scratch[2].at[j], temporal)
    for j in range(len(xs)):
        head_mix(values[j], scratch[2].at[j], scratch[3].at[j], temporal)
    return [(x + dot(scratch[3][j], wo[l], TN)).astype(BF16) for j, x in enumerate(xs)]


def attend(xs, l, norms, wq, wo, scratch, temporal):
    values = []
    for j, x in enumerate(xs):
        a = layer_norm(x, norms[l, 0:1, :], norms[l, 1:2, :])
        qT = dot(wq[l, 0:384, :], a, NT).astype(BF16)
        k = dot(a, wq[l, 384:768, :], NT).astype(BF16)
        values.append(dot(wq[l, 768:1152, :], a, NT).astype(BF16))
        head_scores(qT, k, scratch[0].at[j], temporal)
    return attend_end(xs, values, l, wo, scratch, temporal)


def mlp(res, l, norms, wu, wd, hid):
    res = res.astype(F32)
    a = layer_norm(res, norms[l, 2:3, :], norms[l, 3:4, :])
    for c in range(0, HIDDEN, 512):
        hid[:, c:c + 512] = gelu(dot(a, wu[l, :, c:c + 512], NN))
    return res + dot(hid[...], wd[l], NN)


def kernel(x_hbm, norms, wq_hbm, wo_hbm, wu_hbm, wd_hbm, y_hbm,
           xb, wq, wo, wu, wd, hid, res, sent0, cols1, sent1, frames2, sent2, cols3, yb, normed, queries, keys,
           load_sem, send_sem, recv_sem, *scratch):
    me = lax.axis_index('sp')
    pairs = ((wq_hbm, wq), (wo_hbm, wo), (wu_hbm, wu), (wd_hbm, wd))
    loads = [[pltpu.make_async_copy(s.at[l], d.at[l], load_sem.at[l, i]) for i, (s, d) in enumerate(pairs)]
             for l in range(4)]
    x_load = pltpu.make_async_copy(x_hbm, xb, load_sem.at[4, 0])
    x_load.start()
    for c in loads[0][:2]:
        c.start()
    barrier = pltpu.get_barrier_semaphore()
    for d in range(1, 4):
        pl.semaphore_signal(barrier, inc=1, device_id={'sp': (me + d) % 4}, device_id_type=MESH)
    pl.semaphore_wait(barrier, 3)

    def to_columns(e, src, dst, g, d):
        peer = (me + d) % 4
        return pltpu.make_async_remote_copy(
            src_ref=src.at[g, peer], dst_ref=dst.at[g, pl.ds(4 * me, 4)],
            send_sem=send_sem.at[e, g, d - 1], recv_sem=recv_sem.at[e, g, d - 1],
            device_id={'sp': peer}, device_id_type=MESH)

    def to_frames(e, src, dst, g, d):
        peer = (me + d) % 4
        return pltpu.make_async_remote_copy(
            src_ref=src.at[g, pl.ds(4 * peer, 4)], dst_ref=dst.at[me, g],
            send_sem=send_sem.at[e, g, d - 1], recv_sem=recv_sem.at[e, g, d - 1],
            device_id={'sp': peer}, device_id_type=MESH)

    def keep_rows(rows):
        for f in range(4):
            res[f] = rows[f].reshape(4, 4, 16, WIDTH)

    def prepare_group(g, _):
        for d in (1, 2, 3):
            to_frames(1, sent1, frames2, g, d).wait_recv()
        x = frames2[:, g].reshape(256, WIDTH).astype(F32)
        a = layer_norm(x, norms[2, 0:1, :], norms[2, 1:2, :])
        normed[:, g] = a.reshape(4, 4, 16, WIDTH)
        qk = dot(a, wq[2, 0:768, :], NT).astype(BF16)
        queries[:, g] = qk[:, 0:384].reshape(4, 4, 16, WIDTH)
        keys[:, g] = qk[:, 384:768].reshape(4, 4, 16, WIDTH)
        return 0

    def attend_prepared(l):
        xs, values = [], []
        for f in range(4):
            frame = lambda ref: ref[:, :, f].reshape(256, WIDTH)
            xs.append(frame(frames2).astype(F32))
            values.append(dot(wq[l, 768:1152, :], frame(normed), NT).astype(BF16))
            head_scores_rows(frame(queries), frame(keys), scratch[0].at[f])
        keep_rows(attend_end(xs, values, l, wo, scratch, False))

    def spatial_mlp(l, e, sent, dst):
        def mlp_group(g, _):
            rows = jnp.stack([res[:, j, g] for j in range(4)])
            z = mlp(rows.reshape(256, WIDTH), l, norms, wu, wd, hid)
            sent[g] = z.astype(BF16).reshape(4, 4, 16, WIDTH)
            for d in (2, 1, 3):
                to_columns(e, sent, dst, g, d).start()
            dst[g, pl.ds(4 * me, 4)] = sent[g, me]
            return 0

        lax.fori_loop(0, 4, mlp_group, 0)

    def temporal(l, e, src, write):
        def body(g, _):
            for d in (1, 2, 3):
                to_columns(e, sent0, src, g, d).wait_recv()
            x = swap_halves(src[g].reshape(256, WIDTH).astype(F32), 16, 2)
            rows = attend([x], l, norms, wq, wo, scratch, True)
            z = mlp(rows[0], l, norms, wu, wd, hid)
            write(g, swap_halves(z, 2, 16).astype(BF16).reshape(16, 16, WIDTH))
            return 0
        lax.fori_loop(0, 4, body, 0)

    def send_to_frames(g, z):
        sent1[g] = z
        for d in (2, 1, 3):
            to_frames(1, sent1, frames2, g, d).start()
        frames2[me, g] = sent1[g, pl.ds(4 * me, 4)]

    def y_store(g):
        return pltpu.make_async_copy(yb.at[g], y_hbm.at[:, pl.ds(pl.multiple_of(16 * g, 16), 16), :],
                                     load_sem.at[5, g])

    def write_y(g, z):
        yb[g] = z
        y_store(g).start()

    def wait_weights(l):
        for c in loads[l]:
            c.wait()

    x_load.wait()
    for c in loads[0][:2]:
        c.wait()
    for c in loads[0][2:] + loads[1] + loads[2] + loads[3]:
        c.start()
    keep_rows(attend([xb[f].astype(F32) for f in range(4)], 0, norms, wq, wo, scratch, False))
    for c in loads[0][2:]:
        c.wait()
    spatial_mlp(0, 0, sent0, cols1)
    wait_weights(1)
    temporal(1, 0, cols1, send_to_frames)
    wait_weights(2)
    lax.fori_loop(0, 4, prepare_group, 0)
    attend_prepared(2)
    spatial_mlp(2, 2, sent2, cols3)
    wait_weights(3)
    temporal(3, 2, cols3, write_y)
    for g in range(4):
        y_store(g).wait()
        for d in (1, 2, 3):
            to_columns(0, sent0, cols1, g, d).wait_send()
            to_frames(1, sent1, frames2, g, d).wait_send()
            to_columns(2, sent2, cols3, g, d).wait_send()


def solution(mesh):
    anyspace = pl.BlockSpec(memory_space=pl.ANY)

    def local_stack(latents, norms, w_qkv, w_out, w_up, w_down):
        tokens = (4, 4, 4, 16, WIDTH)
        groups = (4, 16, 16, WIDTH)
        out = pl.pallas_call(
            kernel,
            out_shape=jax.ShapeDtypeStruct((16, 64, WIDTH), BF16),
            in_specs=[anyspace, pl.BlockSpec(memory_space=pltpu.VMEM)] + [anyspace] * 4,
            out_specs=anyspace,
            scratch_shapes=[
                pltpu.VMEM((4, 256, WIDTH), BF16),
                pltpu.VMEM((4, 1152, WIDTH), BF16), pltpu.VMEM((4, WIDTH, WIDTH), BF16),
                pltpu.VMEM((4, WIDTH, HIDDEN), BF16), pltpu.VMEM((4, HIDDEN, WIDTH), BF16),
                pltpu.VMEM((256, HIDDEN), BF16),
                pltpu.VMEM(tokens, BF16),
                pltpu.VMEM(tokens, BF16), pltpu.VMEM(groups, BF16),
                pltpu.VMEM(groups, BF16), pltpu.VMEM(tokens, BF16),
                pltpu.VMEM(tokens, BF16), pltpu.VMEM(groups, BF16),
                pltpu.VMEM(groups, BF16),
                pltpu.VMEM(tokens, BF16), pltpu.VMEM(tokens, BF16), pltpu.VMEM(tokens, BF16),
                pltpu.SemaphoreType.DMA((6, 4)),
                pltpu.SemaphoreType.DMA((3, 4, 3)),
                pltpu.SemaphoreType.DMA((3, 4, 3)),
                pltpu.VMEM((4, 6, 256, 256), F32), pltpu.VMEM((4, 6, 256, 256), F32),
                pltpu.VMEM((4, 6, 256, 256), BF16), pltpu.VMEM((4, WIDTH, 256), BF16),
            ],
            compiler_params=pltpu.CompilerParams(collective_id=0, has_side_effects=True, vmem_limit_bytes=56 * 2**20),
        )(latents[0], norms,
          w_qkv.transpose(0, 2, 3, 4, 1).reshape(4, 3 * WIDTH, WIDTH),
          w_out.reshape(4, WIDTH, WIDTH), w_up, w_down)
        return out[None]

    whole = P()
    return jax.shard_map(local_stack, mesh=mesh,
                         in_specs=(P('data', 'sp', None, None), whole, whole, whole, whole, whole),
                         out_specs=P('data', None, 'sp', None), check_vma=False)
```

```python
import jax
import jax.numpy as jnp
from jax import lax
from jax.experimental import pallas as pl
from jax.experimental.pallas import tpu as pltpu
from jax.sharding import PartitionSpec as P

F32, BF16 = jnp.float32, jnp.bfloat16
EPS = 1e-6
WIDTH, HIDDEN = 384, 1536
NT = (((1,), (1,)), ((), ()))
NN = (((1,), (0,)), ((), ()))
TN = (((0,), (0,)), ((), ()))
SCORE_SCALE = 0.125 * 1.4426950408889634
MESH = pl.DeviceIdType.MESH


def dot(a, b, dims):
    return lax.dot_general(a, b, dims, preferred_element_type=F32)


def layer_norm(x, gain, shift):
    centered = x - jnp.sum(x, -1, keepdims=True) * (1.0 / WIDTH)
    variance = jnp.sum(centered * centered, -1, keepdims=True) * (1.0 / WIDTH)
    return (centered * lax.rsqrt(variance + EPS) * gain + shift).astype(BF16)


def gelu(x):
    c = 0.7978845608028654
    half = 0.5 * x
    return (half + half * jnp.tanh(x * (c + (c * 0.044715) * (x * x)))).astype(BF16)


def swap_halves(x, a, b):
    return x.reshape(a, b, 8, WIDTH).transpose(1, 0, 2, 3).reshape(256, WIDTH)


def head_scores(qT, k, scores, temporal):
    if not temporal:
        zero = jnp.zeros((64, 256), BF16)
        for h in range(6):
            qh = qT[64 * h:64 * h + 64, :]
            rhs = jnp.concatenate([zero, qh] if h % 2 else [qh, zero], 0)
            p = h // 2 * 128
            scores[h] = dot(k[:, p:p + 128], rhs, NN)
    else:
        zero = jnp.zeros((64, 128), BF16)
        row = lax.broadcasted_iota(jnp.int32, (128, 256), 0)
        col = lax.broadcasted_iota(jnp.int32, (128, 256), 1)
        same_patch = (row & 7) == (col & 7)
        for h in range(6):
            p, t = h // 2 * 128, h % 2 * 128
            q0 = jnp.concatenate([qT[p:p + 64, t:t + 128], zero], 1)
            q1 = jnp.concatenate([zero, qT[p + 64:p + 128, t:t + 128]], 1)
            s = dot(k[t:t + 128, p:p + 128], jnp.concatenate([q0, q1], 0), NN)
            scores[h, 0:128] = jnp.where(same_patch, s, -jnp.inf)


def head_probs(scores, expd, probs, temporal):
    keys = 128 if temporal else 256
    for h in range(6):
        peak = jnp.max(scores[h, 0:keys], 0, keepdims=True)
        e = jnp.exp2((scores[h, 0:keys] - peak) * SCORE_SCALE)
        expd[h, 0:keys] = e
        inverse = 1.0 / jnp.sum(e, 0, keepdims=True)
        probs[h, 0:keys] = (expd[h, 0:keys] * inverse).astype(BF16)


def head_mix(vT, probs, mixed, temporal):
    for h in range(6):
        if not temporal:
            r = 64 * h
            mixed[r:r + 64, :] = dot(vT[r:r + 64, :], probs[h], NN).astype(BF16)
        else:
            p, t = h // 2 * 128, h % 2 * 128
            o = dot(vT[p:p + 128, t:t + 128], probs[h, 0:128], NN).astype(BF16)
            mixed[p:p + 64, t:t + 128] = o[0:64, 0:128]
            mixed[p + 64:p + 128, t:t + 128] = o[64:128, 128:256]


def head_scores_rows(q, k, scores):
    low = lax.broadcasted_iota(jnp.int32, (256, 128), 1) < 64
    for h in range(6):
        p = h // 2 * 128
        qp = q[:, p:p + 128]
        zero = jnp.zeros_like(qp)
        rhs = jnp.where(low, zero, qp) if h % 2 else jnp.where(low, qp, zero)
        scores[h] = dot(k[:, p:p + 128], rhs, NT)


def attend_end(xs, values, l, wo, scratch, temporal):
    for j in range(len(xs)):
        head_probs(scratch[0].at[j], scratch[1].at[j], scratch[2].at[j], temporal)
    for j in range(len(xs)):
        head_mix(values[j], scratch[2].at[j], scratch[3].at[j], temporal)
    return [(x + dot(scratch[3][j], wo[l], TN)).astype(BF16) for j, x in enumerate(xs)]


def attend(xs, l, norms, wq, wo, scratch, temporal):
    values = []
    for j, x in enumerate(xs):
        a = layer_norm(x, norms[l, 0:1, :], norms[l, 1:2, :])
        qT = dot(wq[l, 0:384, :], a, NT).astype(BF16)
        k = dot(a, wq[l, 384:768, :], NT).astype(BF16)
        values.append(dot(wq[l, 768:1152, :], a, NT).astype(BF16))
        head_scores(qT, k, scratch[0].at[j], temporal)
    return attend_end(xs, values, l, wo, scratch, temporal)


def mlp(res, l, norms, wu, wd, hid):
    res = res.astype(F32)
    a = layer_norm(res, norms[l, 2:3, :], norms[l, 3:4, :])
    for c in range(0, HIDDEN, 512):
        hid[:, c:c + 512] = gelu(dot(a, wu[l, :, c:c + 512], NN))
    return res + dot(hid[...], wd[l], NN)


def kernel(x_hbm, norms_hbm, wq_hbm, wo_hbm, wu_hbm, wd_hbm, y_hbm,
           xb, norms, wq, wo, wu, wd, hid, res, sent0, cols1, sent1, frames2, sent2, cols3, normed, queries, keys,
           load_sem, send_sem, recv_sem, *scratch):
    me = lax.axis_index('sp')
    pairs = ((wq_hbm, wq), (wo_hbm, wo), (wu_hbm, wu), (wd_hbm, wd))
    loads = [[pltpu.make_async_copy(s.at[l], d.at[l], load_sem.at[l, i]) for i, (s, d) in enumerate(pairs)]
             for l in range(4)]
    x_load = pltpu.make_async_copy(x_hbm, xb, load_sem.at[4, 0])
    norms_load = pltpu.make_async_copy(norms_hbm, norms, load_sem.at[4, 1])
    x_load.start()
    norms_load.start()
    for c in loads[0][:2]:
        c.start()
    barrier = pltpu.get_barrier_semaphore()
    for d in range(1, 4):
        pl.semaphore_signal(barrier, inc=1, device_id={'sp': (me + d) % 4}, device_id_type=MESH)

    def to_columns(e, src, dst, g, d):
        peer = (me + d) % 4
        return pltpu.make_async_remote_copy(
            src_ref=src.at[g, peer], dst_ref=dst.at[g, pl.ds(4 * me, 4)],
            send_sem=send_sem.at[e, g, d - 1], recv_sem=recv_sem.at[e, g, d - 1],
            device_id={'sp': peer}, device_id_type=MESH)

    def to_frames(e, src, dst, g, d):
        peer = (me + d) % 4
        return pltpu.make_async_remote_copy(
            src_ref=src.at[g, pl.ds(4 * peer, 4)], dst_ref=dst.at[me, g],
            send_sem=send_sem.at[e, g, d - 1], recv_sem=recv_sem.at[e, g, d - 1],
            device_id={'sp': peer}, device_id_type=MESH)

    def keep_rows(rows):
        for f in range(4):
            res[f] = rows[f].reshape(4, 4, 16, WIDTH)

    def prepare_group(g, _):
        for d in (1, 2, 3):
            to_frames(1, sent1, frames2, g, d).wait_recv()
        x = frames2[:, g].reshape(256, WIDTH).astype(F32)
        a = layer_norm(x, norms[2, 0:1, :], norms[2, 1:2, :])
        normed[:, g] = a.reshape(4, 4, 16, WIDTH)
        qk = dot(a, wq[2, 0:768, :], NT).astype(BF16)
        queries[:, g] = qk[:, 0:384].reshape(4, 4, 16, WIDTH)
        keys[:, g] = qk[:, 384:768].reshape(4, 4, 16, WIDTH)
        return 0

    def attend_prepared(l):
        xs, values = [], []
        for f in range(4):
            frame = lambda ref: ref[:, :, f].reshape(256, WIDTH)
            xs.append(frame(frames2).astype(F32))
            values.append(dot(wq[l, 768:1152, :], frame(normed), NT).astype(BF16))
            head_scores_rows(frame(queries), frame(keys), scratch[0].at[f])
        keep_rows(attend_end(xs, values, l, wo, scratch, False))

    def spatial_mlp(l, e, sent, dst):
        def mlp_group(g, _):
            rows = jnp.stack([res[:, j, g] for j in range(4)])
            z = mlp(rows.reshape(256, WIDTH), l, norms, wu, wd, hid)
            sent[g] = z.astype(BF16).reshape(4, 4, 16, WIDTH)
            for d in (2, 1, 3):
                to_columns(e, sent, dst, g, d).start()
            dst[g, pl.ds(4 * me, 4)] = sent[g, me]
            return 0

        lax.fori_loop(0, 4, mlp_group, 0)

    def temporal(l, e, src, write):
        def body(g, _):
            for d in (1, 2, 3):
                to_columns(e, sent0, src, g, d).wait_recv()
            x = swap_halves(src[g].reshape(256, WIDTH).astype(F32), 16, 2)
            rows = attend([x], l, norms, wq, wo, scratch, True)
            z = mlp(rows[0], l, norms, wu, wd, hid)
            write(g, swap_halves(z, 2, 16).astype(BF16).reshape(16, 16, WIDTH))
            return 0
        lax.fori_loop(0, 4, body, 0)

    def send_to_frames(g, z):
        sent1[g] = z
        for d in (2, 1, 3):
            to_frames(1, sent1, frames2, g, d).start()
        frames2[me, g] = sent1[g, pl.ds(4 * me, 4)]

    def write_y(g, z):
        y_hbm[:, pl.ds(pl.multiple_of(16 * g, 16), 16), :] = z

    def wait_weights(l):
        for c in loads[l]:
            c.wait()

    x_load.wait()
    norms_load.wait()
    for c in loads[0][:2]:
        c.wait()
    for c in loads[0][2:] + loads[1] + loads[2] + loads[3]:
        c.start()
    keep_rows(attend([xb[f].astype(F32) for f in range(4)], 0, norms, wq, wo, scratch, False))
    for c in loads[0][2:]:
        c.wait()
    pl.semaphore_wait(barrier, 3)
    spatial_mlp(0, 0, sent0, cols1)
    wait_weights(1)
    temporal(1, 0, cols1, send_to_frames)
    wait_weights(2)
    lax.fori_loop(0, 4, prepare_group, 0)
    attend_prepared(2)
    spatial_mlp(2, 2, sent2, cols3)
    wait_weights(3)
    temporal(3, 2, cols3, write_y)
    for g in range(4):
        for d in (1, 2, 3):
            to_columns(0, sent0, cols1, g, d).wait_send()
            to_frames(1, sent1, frames2, g, d).wait_send()
            to_columns(2, sent2, cols3, g, d).wait_send()


def solution(mesh):
    anyspace = pl.BlockSpec(memory_space=pltpu.HBM)

    def local_stack(latents, norms, w_qkv, w_out, w_up, w_down):
        tokens = (4, 4, 4, 16, WIDTH)
        groups = (4, 16, 16, WIDTH)
        out = pl.pallas_call(
            kernel,
            out_shape=jax.ShapeDtypeStruct((16, 64, WIDTH), BF16),
            in_specs=[anyspace] * 6,
            out_specs=pl.BlockSpec(memory_space=pltpu.VMEM),
            scratch_shapes=[
                pltpu.VMEM((4, 256, WIDTH), BF16), pltpu.VMEM((4, 4, WIDTH), F32),
                pltpu.VMEM((4, 1152, WIDTH), BF16), pltpu.VMEM((4, WIDTH, WIDTH), BF16),
                pltpu.VMEM((4, WIDTH, HIDDEN), BF16), pltpu.VMEM((4, HIDDEN, WIDTH), BF16),
                pltpu.VMEM((256, HIDDEN), BF16),
                pltpu.VMEM(tokens, BF16),
                pltpu.VMEM(tokens, BF16), pltpu.VMEM(groups, BF16),
                pltpu.VMEM(groups, BF16), pltpu.VMEM(tokens, BF16),
                pltpu.VMEM(tokens, BF16), pltpu.VMEM(groups, BF16),
                pltpu.VMEM(tokens, BF16), pltpu.VMEM(tokens, BF16), pltpu.VMEM(tokens, BF16),
                pltpu.SemaphoreType.DMA((6, 4)),
                pltpu.SemaphoreType.DMA((3, 4, 3)),
                pltpu.SemaphoreType.DMA((3, 4, 3)),
                pltpu.VMEM((4, 6, 256, 256), F32), pltpu.VMEM((4, 6, 256, 256), F32),
                pltpu.VMEM((4, 6, 256, 256), BF16), pltpu.VMEM((4, WIDTH, 256), BF16),
            ],
            compiler_params=pltpu.CompilerParams(collective_id=0, has_side_effects=True, vmem_limit_bytes=48 * 2**20),
        )(*[pltpu.with_memory_space_constraint(a, pltpu.HBM) for a in (
            latents[0], norms,
            w_qkv.transpose(0, 2, 3, 4, 1).reshape(4, 3 * WIDTH, WIDTH),
            w_out.reshape(4, WIDTH, WIDTH), w_up, w_down)])
        return out[None]

    whole = P()
    return jax.shard_map(local_stack, mesh=mesh,
                         in_specs=(P('data', 'sp', None, None), whole, whole, whole, whole, whole),
                         out_specs=P('data', None, 'sp', None), check_vma=False)
```

```python
import jax
import jax.numpy as jnp
from jax import lax
from jax.experimental import pallas as pl
from jax.experimental.pallas import tpu as pltpu
from jax.sharding import PartitionSpec as P

F32, BF16 = jnp.float32, jnp.bfloat16
EPS = 1e-6
WIDTH, HIDDEN = 384, 1536
NT = (((1,), (1,)), ((), ()))
NN = (((1,), (0,)), ((), ()))
TN = (((0,), (0,)), ((), ()))
SCORE_SCALE = 0.125 * 1.4426950408889634
MESH = pl.DeviceIdType.MESH
PAIRED, LATE = (3,), ()


def dot(a, b, dims):
    return lax.dot_general(a, b, dims, preferred_element_type=F32)


def layer_norm(x, gain, shift):
    centered = x - jnp.sum(x, -1, keepdims=True) * (1.0 / WIDTH)
    variance = jnp.sum(centered * centered, -1, keepdims=True) * (1.0 / WIDTH)
    return (centered * lax.rsqrt(variance + EPS) * gain + shift).astype(BF16)


def gelu(x):
    c = 0.7978845608028654
    half = 0.5 * x
    return (half + half * jnp.tanh(x * (c + (c * 0.044715) * (x * x)))).astype(BF16)


def swap_halves(x, a, b):
    return x.reshape(a, b, 8, WIDTH).transpose(1, 0, 2, 3).reshape(256, WIDTH)


def head_scores(qT, k, scores, temporal):
    if not temporal:
        zero = jnp.zeros((64, 256), BF16)
        for h in range(6):
            qh = qT[64 * h:64 * h + 64, :]
            rhs = jnp.concatenate([zero, qh] if h % 2 else [qh, zero], 0)
            p = h // 2 * 128
            scores[h] = dot(k[:, p:p + 128], rhs, NN)
    else:
        zero = jnp.zeros((64, 128), BF16)
        row = lax.broadcasted_iota(jnp.int32, (128, 256), 0)
        col = lax.broadcasted_iota(jnp.int32, (128, 256), 1)
        same_patch = (row & 7) == (col & 7)
        for h in range(6):
            p, t = h // 2 * 128, h % 2 * 128
            q0 = jnp.concatenate([qT[p:p + 64, t:t + 128], zero], 1)
            q1 = jnp.concatenate([zero, qT[p + 64:p + 128, t:t + 128]], 1)
            s = dot(k[t:t + 128, p:p + 128], jnp.concatenate([q0, q1], 0), NN)
            scores[h, 0:128] = jnp.where(same_patch, s, -jnp.inf)


def head_probs(scores, expd, probs, temporal):
    keys = 128 if temporal else 256
    for h in range(6):
        peak = jnp.max(scores[h, 0:keys], 0, keepdims=True)
        e = jnp.exp2((scores[h, 0:keys] - peak) * SCORE_SCALE)
        expd[h, 0:keys] = e
        inverse = 1.0 / jnp.sum(e, 0, keepdims=True)
        probs[h, 0:keys] = (expd[h, 0:keys] * inverse).astype(BF16)


def head_mix(vT, probs, mixed, temporal):
    for h in range(6):
        if not temporal:
            r = 64 * h
            mixed[r:r + 64, :] = dot(vT[r:r + 64, :], probs[h], NN).astype(BF16)
        else:
            p, t = h // 2 * 128, h % 2 * 128
            o = dot(vT[p:p + 128, t:t + 128], probs[h, 0:128], NN).astype(BF16)
            mixed[p:p + 64, t:t + 128] = o[0:64, 0:128]
            mixed[p + 64:p + 128, t:t + 128] = o[64:128, 128:256]


def attend_end(xs, values, l, wo, scratch, temporal):
    for j in range(len(xs)):
        head_probs(scratch[0].at[j], scratch[1].at[j], scratch[2].at[j], temporal)
    for j in range(len(xs)):
        head_mix(values[j], scratch[2].at[j], scratch[3].at[j], temporal)
    return [(x + dot(scratch[3][j], wo[l], TN)).astype(BF16) for j, x in enumerate(xs)]


def attend(xs, l, norms, wq, wo, scratch, temporal):
    values = []
    for j, x in enumerate(xs):
        a = layer_norm(x, norms[l, 0:1, :], norms[l, 1:2, :])
        qT = dot(wq[l, 0:384, :], a, NT).astype(BF16)
        k = dot(a, wq[l, 384:768, :], NT).astype(BF16)
        values.append(dot(wq[l, 768:1152, :], a, NT).astype(BF16))
        head_scores(qT, k, scratch[0].at[j], temporal)
    return attend_end(xs, values, l, wo, scratch, temporal)


def mlp(res, l, norms, wu, wd, hid):
    res = res.astype(F32)
    a = layer_norm(res, norms[l, 2:3, :], norms[l, 3:4, :])
    for c in range(0, HIDDEN, 512):
        hid[:, c:c + 512] = gelu(dot(a, wu[l, :, c:c + 512], NN))
    return res + dot(hid[...], wd[l], NN)


def kernel(x_hbm, norms_hbm, wq_hbm, wo_hbm, wu_hbm, wd_hbm, y_hbm,
           xb, norms, wq, wo, wu, wd, hid, res, sent0, cols1, sent1, frames2, sent2, cols3, normed, queries, keys, values,
           load_sem, send_sem, recv_sem, *scratch):
    me = lax.axis_index('sp')
    pairs = ((wq_hbm, wq), (wo_hbm, wo), (wu_hbm, wu), (wd_hbm, wd))
    loads = [[pltpu.make_async_copy(s.at[l], d.at[l], load_sem.at[l, i]) for i, (s, d) in enumerate(pairs)]
             for l in range(4)]
    x_load = pltpu.make_async_copy(x_hbm, xb, load_sem.at[4, 0])
    norms_load = pltpu.make_async_copy(norms_hbm, norms, load_sem.at[4, 1])
    x_load.start()
    norms_load.start()
    for c in loads[0][:2]:
        c.start()
    barrier = pltpu.get_barrier_semaphore()
    for d in range(1, 4):
        pl.semaphore_signal(barrier, inc=1, device_id={'sp': (me + d) % 4}, device_id_type=MESH)

    def to_columns(e, src, dst, g, d):
        peer = (me + d) % 4
        return pltpu.make_async_remote_copy(
            src_ref=src.at[g, peer], dst_ref=dst.at[g, pl.ds(4 * me, 4)],
            send_sem=send_sem.at[e, g, d - 1], recv_sem=recv_sem.at[e, g, d - 1],
            device_id={'sp': peer}, device_id_type=MESH)

    def to_frames(e, src, dst, g, d):
        peer = (me + d) % 4
        return pltpu.make_async_remote_copy(
            src_ref=src.at[g, pl.ds(4 * peer, 4)], dst_ref=dst.at[me, g],
            send_sem=send_sem.at[e, g, d - 1], recv_sem=recv_sem.at[e, g, d - 1],
            device_id={'sp': peer}, device_id_type=MESH)

    def keep_queries(qk, at):
        queries[at] = qk[:, 0:384].astype(BF16).reshape(4, 4, 16, WIDTH)
        keys[at] = qk[:, 384:768].astype(BF16).reshape(4, 4, 16, WIDTH)

    def prepare_frames():
        for f in range(4):
            a = layer_norm(xb[f].reshape(256, WIDTH).astype(F32), norms[0, 0:1, :], norms[0, 1:2, :])
            keep_queries(dot(a, wq[0, 0:768, :], NT), (slice(None), slice(None), f))
            values[f] = dot(wq[0, 768:1152, :], a, NT).astype(BF16)

    def prepare_group(g, _):
        for d in (1, 2, 3):
            to_frames(1, sent1, frames2, g, d).wait_recv()
        x = frames2[:, g].reshape(256, WIDTH).astype(F32)
        a = layer_norm(x, norms[2, 0:1, :], norms[2, 1:2, :])
        normed[:, g] = a.reshape(4, 4, 16, WIDTH)
        keep_queries(dot(a, wq[2, 0:768, :], NT), (slice(None), g))
        return 0

    def prepare_values():
        for f in range(4):
            values[f] = dot(wq[2, 768:1152, :], normed[:, :, f].reshape(256, WIDTH), NT).astype(BF16)

    def attend_half(l, half, read):
        scores, expd, probs, mixed = scratch
        groups = pl.ds(2 * half, 2)
        low = lax.broadcasted_iota(jnp.int32, (128, 128), 1) < 64
        for f in range(4):
            q = queries[:, groups, f].reshape(128, WIDTH)
            k = keys[:, :, f].reshape(256, WIDTH)
            for p in range(3):
                qp = q[:, 128 * p:128 * p + 128]
                zero = jnp.zeros_like(qp)
                rhs = jnp.concatenate([jnp.where(low, qp, zero), jnp.where(low, zero, qp)], 0)
                scores[f // 2, 3 * (f % 2) + p] = dot(k[:, 128 * p:128 * p + 128], rhs, NT)
        for j in range(2):
            head_probs(scores.at[j], expd.at[j], probs.at[j], False)
        for f in range(4):
            lanes = 128 * (f % 2)
            for p in range(3):
                r = 128 * p
                o = dot(values[f, r:r + 128, :], probs[f // 2, 3 * (f % 2) + p], NN).astype(BF16)
                mixed[f // 2, r:r + 64, lanes:lanes + 128] = o[0:64, 0:128]
                mixed[f // 2, r + 64:r + 128, lanes:lanes + 128] = o[64:128, 128:256]
        for j in range(2):
            x = jnp.concatenate([read(2 * j + u, groups).reshape(128, WIDTH) for u in range(2)], 0)
            rows = (x.astype(F32) + dot(mixed[j], wo[l], TN)).astype(BF16)
            for u in range(2):
                res[2 * j + u, :, groups] = rows[128 * u:128 * u + 128].reshape(4, 2, 16, WIDTH)

    def spatial_rest(l, e, read, sent, dst, before_send):
        def half_step(half, _):
            attend_half(l, half, read)
            def group_mlp(u):
                rows = jnp.stack([res[:, j, 2 * half + u] for j in range(4)])
                z = mlp(rows.reshape(256, WIDTH), l, norms, wu, wd, hid.at[u])
                sent[2 * half + u] = z.astype(BF16).reshape(4, 4, 16, WIDTH)

            def send(u):
                g = 2 * half + u
                for d in (2, 1, 3):
                    to_columns(e, sent, dst, g, d).start()
                dst[g, pl.ds(4 * me, 4)] = sent[g, me]

            if l in LATE:
                for u in range(2):
                    group_mlp(u)
                for u in range(2):
                    send(u)
            else:
                for u in range(2):
                    group_mlp(u)
                    send(u)
            return 0
        before_send()
        lax.fori_loop(0, 2, half_step, 0)

    def temporal(l, e, src, write):
        n = 2 if l in PAIRED else 1

        def body(i, _):
            xs = []
            for j in range(n):
                for d in (1, 2, 3):
                    to_columns(e, sent0, src, n * i + j, d).wait_recv()
            for j in range(n):
                xs.append(swap_halves(src[n * i + j].reshape(256, WIDTH).astype(F32), 16, 2))
            rows = attend(xs, l, norms, wq, wo, scratch, True)
            zs = [mlp(rows[j], l, norms, wu, wd, hid.at[j]) for j in range(n)]
            for j in range(n):
                write(n * i + j, swap_halves(zs[j], 2, 16).astype(BF16).reshape(16, 16, WIDTH))
            return 0
        lax.fori_loop(0, 4 // n, body, 0)

    def send_to_frames(g, z):
        sent1[g] = z
        for d in (2, 1, 3):
            to_frames(1, sent1, frames2, g, d).start()
        frames2[me, g] = sent1[g, pl.ds(4 * me, 4)]

    def write_y(g, z):
        y_hbm[:, pl.ds(pl.multiple_of(16 * g, 16), 16), :] = z

    def wait_weights(l):
        for c in loads[l]:
            c.wait()

    x_load.wait()
    norms_load.wait()
    for c in loads[0][:2]:
        c.wait()
    for c in loads[0][2:] + loads[1] + loads[2] + loads[3]:
        c.start()
    prepare_frames()

    def block0_ready():
        for c in loads[0][2:]:
            c.wait()
        pl.semaphore_wait(barrier, 3)

    spatial_rest(0, 0, lambda f, groups: xb[f, :, groups], sent0, cols1, block0_ready)
    wait_weights(1)
    temporal(1, 0, cols1, send_to_frames)
    wait_weights(2)
    lax.fori_loop(0, 4, prepare_group, 0)
    prepare_values()
    spatial_rest(2, 2, lambda f, groups: frames2[:, groups, f], sent2, cols3, lambda: None)
    wait_weights(3)
    temporal(3, 2, cols3, write_y)
    for g in range(4):
        for d in (1, 2, 3):
            to_columns(0, sent0, cols1, g, d).wait_send()
            to_frames(1, sent1, frames2, g, d).wait_send()
            to_columns(2, sent2, cols3, g, d).wait_send()


def solution(mesh):
    anyspace = pl.BlockSpec(memory_space=pltpu.HBM)

    def local_stack(latents, norms, w_qkv, w_out, w_up, w_down):
        tokens = (4, 4, 4, 16, WIDTH)
        groups = (4, 16, 16, WIDTH)
        out = pl.pallas_call(
            kernel,
            out_shape=jax.ShapeDtypeStruct((16, 64, WIDTH), BF16),
            in_specs=[anyspace] * 6,
            out_specs=pl.BlockSpec(memory_space=pltpu.VMEM),
            scratch_shapes=[
                pltpu.VMEM(tokens, BF16), pltpu.VMEM((4, 4, WIDTH), F32),
                pltpu.VMEM((4, 1152, WIDTH), BF16), pltpu.VMEM((4, WIDTH, WIDTH), BF16),
                pltpu.VMEM((4, WIDTH, HIDDEN), BF16), pltpu.VMEM((4, HIDDEN, WIDTH), BF16),
                pltpu.VMEM((2, 256, HIDDEN), BF16),
                pltpu.VMEM(tokens, BF16),
                pltpu.VMEM(tokens, BF16), pltpu.VMEM(groups, BF16),
                pltpu.VMEM(groups, BF16), pltpu.VMEM(tokens, BF16),
                pltpu.VMEM(tokens, BF16), pltpu.VMEM(groups, BF16),
                pltpu.VMEM(tokens, BF16), pltpu.VMEM(tokens, BF16), pltpu.VMEM(tokens, BF16),
                pltpu.VMEM((4, WIDTH, 256), BF16),
                pltpu.SemaphoreType.DMA((6, 4)),
                pltpu.SemaphoreType.DMA((3, 4, 3)),
                pltpu.SemaphoreType.DMA((3, 4, 3)),
                pltpu.VMEM((2, 6, 256, 256), F32), pltpu.VMEM((2, 6, 256, 256), F32),
                pltpu.VMEM((2, 6, 256, 256), BF16), pltpu.VMEM((2, WIDTH, 256), BF16),
            ],
            compiler_params=pltpu.CompilerParams(collective_id=0, has_side_effects=True, vmem_limit_bytes=48 * 2**20),
        )(*[pltpu.with_memory_space_constraint(a, pltpu.HBM) for a in (
            latents.reshape(tokens), norms,
            w_qkv.transpose(0, 2, 3, 4, 1).reshape(4, 3 * WIDTH, WIDTH),
            w_out.reshape(4, WIDTH, WIDTH), w_up, w_down)])
        return out[None]

    whole = P()
    return jax.shard_map(local_stack, mesh=mesh,
                         in_specs=(P('data', 'sp', None, None), whole, whole, whole, whole, whole),
                         out_specs=P('data', None, 'sp', None), check_vma=False)
```

```python
import jax
import jax.numpy as jnp
from jax import lax
from jax.experimental import pallas as pl
from jax.experimental.pallas import tpu as pltpu
from jax.sharding import PartitionSpec as P

F32, BF16 = jnp.float32, jnp.bfloat16
EPS = 1e-6
WIDTH, HIDDEN = 384, 1536
NT = (((1,), (1,)), ((), ()))
NN = (((1,), (0,)), ((), ()))
TN = (((0,), (0,)), ((), ()))
SCORE_SCALE = 0.125 * 1.4426950408889634
MESH = pl.DeviceIdType.MESH
PAIRED, LATE = (3,), ()


def dot(a, b, dims):
    return lax.dot_general(a, b, dims, preferred_element_type=F32)


def layer_norm(x, gain, shift):
    centered = x - jnp.sum(x, -1, keepdims=True) * (1.0 / WIDTH)
    variance = jnp.sum(centered * centered, -1, keepdims=True) * (1.0 / WIDTH)
    return (centered * lax.rsqrt(variance + EPS) * gain + shift).astype(BF16)


def gelu_of_half(h):
    c = 0.7978845608028654
    return (h + h * jnp.tanh(h * (2.0 * c + (8.0 * c * 0.044715) * (h * h)))).astype(BF16)


def swap_halves(x, a, b):
    return x.reshape(a, b, 8, WIDTH).transpose(1, 0, 2, 3).reshape(256, WIDTH)


def head_scores(qT, k, scores, temporal):
    if not temporal:
        zero = jnp.zeros((64, 256), BF16)
        for h in range(6):
            qh = qT[64 * h:64 * h + 64, :]
            rhs = jnp.concatenate([zero, qh] if h % 2 else [qh, zero], 0)
            p = h // 2 * 128
            scores[h] = dot(k[:, p:p + 128], rhs, NN)
    else:
        zero = jnp.zeros((64, 128), BF16)
        row = lax.broadcasted_iota(jnp.int32, (128, 256), 0)
        col = lax.broadcasted_iota(jnp.int32, (128, 256), 1)
        same_patch = (row & 7) == (col & 7)
        for h in range(6):
            p, t = h // 2 * 128, h % 2 * 128
            q0 = jnp.concatenate([qT[p:p + 64, t:t + 128], zero], 1)
            q1 = jnp.concatenate([zero, qT[p + 64:p + 128, t:t + 128]], 1)
            s = dot(k[t:t + 128, p:p + 128], jnp.concatenate([q0, q1], 0), NN)
            scores[h, 0:128] = jnp.where(same_patch, s, -jnp.inf)


def head_probs(scores, expd, probs, temporal):
    keys = 128 if temporal else 256
    for h in range(6):
        peak = jnp.max(scores[h, 0:keys], 0, keepdims=True)
        e = jnp.exp2((scores[h, 0:keys] - peak) * SCORE_SCALE)
        expd[h, 0:keys] = e
        inverse = 1.0 / jnp.sum(e, 0, keepdims=True)
        probs[h, 0:keys] = (expd[h, 0:keys] * inverse).astype(BF16)


def head_mix(vT, probs, mixed, temporal):
    for h in range(6):
        if not temporal:
            r = 64 * h
            mixed[r:r + 64, :] = dot(vT[r:r + 64, :], probs[h], NN).astype(BF16)
        else:
            p, t = h // 2 * 128, h % 2 * 128
            o = dot(vT[p:p + 128, t:t + 128], probs[h, 0:128], NN).astype(BF16)
            mixed[p:p + 64, t:t + 128] = o[0:64, 0:128]
            mixed[p + 64:p + 128, t:t + 128] = o[64:128, 128:256]


def attend_end(xs, values, l, wo, scratch, temporal):
    for j in range(len(xs)):
        head_probs(scratch[0].at[j], scratch[1].at[j], scratch[2].at[j], temporal)
    for j in range(len(xs)):
        head_mix(values[j], scratch[2].at[j], scratch[3].at[j], temporal)
    return [(x + dot(scratch[3][j], wo[l], TN)).astype(BF16) for j, x in enumerate(xs)]


def attend(xs, l, norms, wq, wo, scratch, temporal):
    values = []
    for j, x in enumerate(xs):
        a = layer_norm(x, norms[l, 0:1, :], norms[l, 1:2, :])
        qT = dot(wq[l, 0:384, :], a, NT).astype(BF16)
        k = dot(a, wq[l, 384:768, :], NT).astype(BF16)
        values.append(dot(wq[l, 768:1152, :], a, NT).astype(BF16))
        head_scores(qT, k, scratch[0].at[j], temporal)
    return attend_end(xs, values, l, wo, scratch, temporal)


def mlp(res, l, norms, wu, wd, hid):
    res = res.astype(F32)
    half = layer_norm(res, 0.5 * norms[l, 2:3, :], 0.5 * norms[l, 3:4, :])
    for c in range(0, HIDDEN, 512):
        hid[:, c:c + 512] = gelu_of_half(dot(half, wu[l, :, c:c + 512], NN))
    return res + dot(hid[...], wd[l], NN)


def kernel(x_hbm, norms_hbm, wq_hbm, wo_hbm, wu_hbm, wd_hbm, y_hbm,
           xb, norms, wq, wo, wu, wd, hid, res, sent0, cols1, sent1, frames2, sent2, cols3, normed, queries, keys, values,
           load_sem, send_sem, recv_sem, *scratch):
    me = lax.axis_index('sp')
    pairs = ((wq_hbm, wq), (wo_hbm, wo), (wu_hbm, wu), (wd_hbm, wd))
    loads = [[pltpu.make_async_copy(s.at[l], d.at[l], load_sem.at[l, i]) for i, (s, d) in enumerate(pairs)]
             for l in range(4)]
    x_load = pltpu.make_async_copy(x_hbm, xb, load_sem.at[4, 0])
    norms_load = pltpu.make_async_copy(norms_hbm, norms, load_sem.at[4, 1])
    x_load.start()
    norms_load.start()
    for c in loads[0][:2]:
        c.start()
    barrier = pltpu.get_barrier_semaphore()
    for d in range(1, 4):
        pl.semaphore_signal(barrier, inc=1, device_id={'sp': (me + d) % 4}, device_id_type=MESH)

    def to_columns(e, src, dst, g, d):
        peer = (me + d) % 4
        return pltpu.make_async_remote_copy(
            src_ref=src.at[g, peer], dst_ref=dst.at[g, pl.ds(4 * me, 4)],
            send_sem=send_sem.at[e, g, d - 1], recv_sem=recv_sem.at[e, g, d - 1],
            device_id={'sp': peer}, device_id_type=MESH)

    def to_frames(e, src, dst, g, d):
        peer = (me + d) % 4
        return pltpu.make_async_remote_copy(
            src_ref=src.at[g, pl.ds(4 * peer, 4)], dst_ref=dst.at[me, g],
            send_sem=send_sem.at[e, g, d - 1], recv_sem=recv_sem.at[e, g, d - 1],
            device_id={'sp': peer}, device_id_type=MESH)

    def keep_queries(qk, at):
        queries[at] = qk[:, 0:384].astype(BF16).reshape(4, 4, 16, WIDTH)
        keys[at] = qk[:, 384:768].astype(BF16).reshape(4, 4, 16, WIDTH)

    def prepare_frames():
        for f in range(4):
            a = layer_norm(xb[f].reshape(256, WIDTH).astype(F32), norms[0, 0:1, :], norms[0, 1:2, :])
            keep_queries(dot(a, wq[0, 0:768, :], NT), (slice(None), slice(None), f))
            values[f] = dot(wq[0, 768:1152, :], a, NT).astype(BF16)

    def prepare_group(g, _):
        for d in (1, 2, 3):
            to_frames(1, sent1, frames2, g, d).wait_recv()
        x = frames2[:, g].reshape(256, WIDTH).astype(F32)
        a = layer_norm(x, norms[2, 0:1, :], norms[2, 1:2, :])
        normed[:, g] = a.reshape(4, 4, 16, WIDTH)
        keep_queries(dot(a, wq[2, 0:768, :], NT), (slice(None), g))
        return 0

    def prepare_values():
        for f in range(4):
            values[f] = dot(wq[2, 768:1152, :], normed[:, :, f].reshape(256, WIDTH), NT).astype(BF16)

    def attend_half(l, half, read):
        scores, expd, probs, mixed = scratch
        groups = pl.ds(2 * half, 2)
        low = lax.broadcasted_iota(jnp.int32, (128, 128), 1) < 64
        for f in range(4):
            q = queries[:, groups, f].reshape(128, WIDTH)
            k = keys[:, :, f].reshape(256, WIDTH)
            for p in range(3):
                qp = q[:, 128 * p:128 * p + 128]
                zero = jnp.zeros_like(qp)
                rhs = jnp.concatenate([jnp.where(low, qp, zero), jnp.where(low, zero, qp)], 0)
                scores[f // 2, 3 * (f % 2) + p] = dot(k[:, 128 * p:128 * p + 128], rhs, NT)
        for j in range(2):
            head_probs(scores.at[j], expd.at[j], probs.at[j], False)
        for f in range(4):
            lanes = 128 * (f % 2)
            for p in range(3):
                r = 128 * p
                o = dot(values[f, r:r + 128, :], probs[f // 2, 3 * (f % 2) + p], NN).astype(BF16)
                mixed[f // 2, r:r + 64, lanes:lanes + 128] = o[0:64, 0:128]
                mixed[f // 2, r + 64:r + 128, lanes:lanes + 128] = o[64:128, 128:256]
        for j in range(2):
            x = jnp.concatenate([read(2 * j + u, groups).reshape(128, WIDTH) for u in range(2)], 0)
            rows = (x.astype(F32) + dot(mixed[j], wo[l], TN)).astype(BF16)
            for u in range(2):
                res[2 * j + u, :, groups] = rows[128 * u:128 * u + 128].reshape(4, 2, 16, WIDTH)

    def spatial_rest(l, e, read, sent, dst, before_send):
        def half_step(half, _):
            attend_half(l, half, read)
            def group_mlp(u):
                rows = jnp.stack([res[:, j, 2 * half + u] for j in range(4)])
                z = mlp(rows.reshape(256, WIDTH), l, norms, wu, wd, hid.at[u])
                sent[2 * half + u] = z.astype(BF16).reshape(4, 4, 16, WIDTH)

            def send(u):
                g = 2 * half + u
                for d in (2, 1, 3):
                    to_columns(e, sent, dst, g, d).start()
                dst[g, pl.ds(4 * me, 4)] = sent[g, me]

            if l in LATE:
                for u in range(2):
                    group_mlp(u)
                for u in range(2):
                    send(u)
            else:
                for u in range(2):
                    group_mlp(u)
                    send(u)
            return 0
        before_send()
        lax.fori_loop(0, 2, half_step, 0)

    def temporal(l, e, src, write):
        n = 2 if l in PAIRED else 1

        def body(i, _):
            xs = []
            for j in range(n):
                for d in (1, 2, 3):
                    to_columns(e, sent0, src, n * i + j, d).wait_recv()
            for j in range(n):
                xs.append(swap_halves(src[n * i + j].reshape(256, WIDTH).astype(F32), 16, 2))
            rows = attend(xs, l, norms, wq, wo, scratch, True)
            zs = [mlp(rows[j], l, norms, wu, wd, hid.at[j]) for j in range(n)]
            for j in range(n):
                write(n * i + j, swap_halves(zs[j], 2, 16).astype(BF16).reshape(16, 16, WIDTH))
            return 0
        lax.fori_loop(0, 4 // n, body, 0)

    def send_to_frames(g, z):
        sent1[g] = z
        for d in (2, 1, 3):
            to_frames(1, sent1, frames2, g, d).start()
        frames2[me, g] = sent1[g, pl.ds(4 * me, 4)]

    def write_y(g, z):
        y_hbm[:, pl.ds(pl.multiple_of(16 * g, 16), 16), :] = z

    def wait_weights(l):
        for c in loads[l]:
            c.wait()

    x_load.wait()
    norms_load.wait()
    for c in loads[0][:2]:
        c.wait()
    for c in loads[0][2:] + loads[1] + loads[2] + loads[3]:
        c.start()
    prepare_frames()

    def block0_ready():
        for c in loads[0][2:]:
            c.wait()
        pl.semaphore_wait(barrier, 3)

    spatial_rest(0, 0, lambda f, groups: xb[f, :, groups], sent0, cols1, block0_ready)
    wait_weights(1)
    temporal(1, 0, cols1, send_to_frames)
    wait_weights(2)
    lax.fori_loop(0, 4, prepare_group, 0)
    prepare_values()
    spatial_rest(2, 2, lambda f, groups: frames2[:, groups, f], sent2, cols3, lambda: None)
    wait_weights(3)
    temporal(3, 2, cols3, write_y)
    for g in range(4):
        for d in (1, 2, 3):
            to_columns(0, sent0, cols1, g, d).wait_send()
            to_frames(1, sent1, frames2, g, d).wait_send()
            to_columns(2, sent2, cols3, g, d).wait_send()


def solution(mesh):
    anyspace = pl.BlockSpec(memory_space=pltpu.HBM)

    def local_stack(latents, norms, w_qkv, w_out, w_up, w_down):
        tokens = (4, 4, 4, 16, WIDTH)
        groups = (4, 16, 16, WIDTH)
        out = pl.pallas_call(
            kernel,
            out_shape=jax.ShapeDtypeStruct((16, 64, WIDTH), BF16),
            in_specs=[anyspace] * 6,
            out_specs=pl.BlockSpec(memory_space=pltpu.VMEM),
            scratch_shapes=[
                pltpu.VMEM(tokens, BF16), pltpu.VMEM((4, 4, WIDTH), F32),
                pltpu.VMEM((4, 1152, WIDTH), BF16), pltpu.VMEM((4, WIDTH, WIDTH), BF16),
                pltpu.VMEM((4, WIDTH, HIDDEN), BF16), pltpu.VMEM((4, HIDDEN, WIDTH), BF16),
                pltpu.VMEM((2, 256, HIDDEN), BF16),
                pltpu.VMEM(tokens, BF16),
                pltpu.VMEM(tokens, BF16), pltpu.VMEM(groups, BF16),
                pltpu.VMEM(groups, BF16), pltpu.VMEM(tokens, BF16),
                pltpu.VMEM(tokens, BF16), pltpu.VMEM(groups, BF16),
                pltpu.VMEM(tokens, BF16), pltpu.VMEM(tokens, BF16), pltpu.VMEM(tokens, BF16),
                pltpu.VMEM((4, WIDTH, 256), BF16),
                pltpu.SemaphoreType.DMA((6, 4)),
                pltpu.SemaphoreType.DMA((3, 4, 3)),
                pltpu.SemaphoreType.DMA((3, 4, 3)),
                pltpu.VMEM((2, 6, 256, 256), F32), pltpu.VMEM((2, 6, 256, 256), F32),
                pltpu.VMEM((2, 6, 256, 256), BF16), pltpu.VMEM((2, WIDTH, 256), BF16),
            ],
            compiler_params=pltpu.CompilerParams(collective_id=0, has_side_effects=True, vmem_limit_bytes=48 * 2**20),
        )(*[pltpu.with_memory_space_constraint(a, pltpu.HBM) for a in (
            latents.reshape(tokens), norms,
            w_qkv.transpose(0, 2, 3, 4, 1).reshape(4, 3 * WIDTH, WIDTH),
            w_out.reshape(4, WIDTH, WIDTH), w_up, w_down)])
        return out[None]

    whole = P()
    return jax.shard_map(local_stack, mesh=mesh,
                         in_specs=(P('data', 'sp', None, None), whole, whole, whole, whole, whole),
                         out_specs=P('data', None, 'sp', None), check_vma=False)
```

```python
import jax
import jax.numpy as jnp
from jax import lax
from jax.experimental import pallas as pl
from jax.experimental.pallas import tpu as pltpu
from jax.sharding import PartitionSpec as P

F32, BF16 = jnp.float32, jnp.bfloat16
EPS = 1e-6
WIDTH, HIDDEN = 384, 1536
NT = (((1,), (1,)), ((), ()))
NN = (((1,), (0,)), ((), ()))
TN = (((0,), (0,)), ((), ()))
SCORE_SCALE = 0.125 * 1.4426950408889634
MESH = pl.DeviceIdType.MESH
PAIRED, LATE = (3,), ()


def dot(a, b, dims):
    return lax.dot_general(a, b, dims, preferred_element_type=F32)


def layer_norm(x, gain, shift):
    centered = x - jnp.sum(x, -1, keepdims=True) * (1.0 / WIDTH)
    variance = jnp.sum(centered * centered, -1, keepdims=True) * (1.0 / WIDTH)
    return (centered * lax.rsqrt(variance + EPS) * gain + shift).astype(BF16)


def gelu_of_half(h):
    c = 0.7978845608028654
    return (h + h * jnp.tanh(h * (2.0 * c + (8.0 * c * 0.044715) * (h * h)))).astype(BF16)


def swap_halves(x, a, b):
    return x.reshape(a, b, 8, WIDTH).transpose(1, 0, 2, 3).reshape(256, WIDTH)


def head_scores(qT, k, scores, temporal):
    if not temporal:
        zero = jnp.zeros((64, 256), BF16)
        for h in range(6):
            qh = qT[64 * h:64 * h + 64, :]
            rhs = jnp.concatenate([zero, qh] if h % 2 else [qh, zero], 0)
            p = h // 2 * 128
            scores[h] = dot(k[:, p:p + 128], rhs, NN)
    else:
        zero = jnp.zeros((64, 128), BF16)
        row = lax.broadcasted_iota(jnp.int32, (128, 256), 0)
        col = lax.broadcasted_iota(jnp.int32, (128, 256), 1)
        same_patch = (row & 7) == (col & 7)
        for h in range(6):
            p, t = h // 2 * 128, h % 2 * 128
            q0 = jnp.concatenate([qT[p:p + 64, t:t + 128], zero], 1)
            q1 = jnp.concatenate([zero, qT[p + 64:p + 128, t:t + 128]], 1)
            s = dot(k[t:t + 128, p:p + 128], jnp.concatenate([q0, q1], 0), NN)
            scores[h, 0:128] = jnp.where(same_patch, s, -jnp.inf)


def head_probs(scores, expd, probs, temporal):
    keys = 128 if temporal else 256
    for h in range(6):
        peak = jnp.max(scores[h, 0:keys], 0, keepdims=True)
        e = jnp.exp2((scores[h, 0:keys] - peak) * SCORE_SCALE)
        expd[h, 0:keys] = e
        inverse = 1.0 / jnp.sum(e, 0, keepdims=True)
        probs[h, 0:keys] = (expd[h, 0:keys] * inverse).astype(BF16)


def head_mix(vT, probs, mixed, temporal):
    for h in range(6):
        if not temporal:
            r = 64 * h
            mixed[r:r + 64, :] = dot(vT[r:r + 64, :], probs[h], NN).astype(BF16)
        else:
            p, t = h // 2 * 128, h % 2 * 128
            o = dot(vT[p:p + 128, t:t + 128], probs[h, 0:128], NN).astype(BF16)
            mixed[p:p + 64, t:t + 128] = o[0:64, 0:128]
            mixed[p + 64:p + 128, t:t + 128] = o[64:128, 128:256]


def attend_end(xs, values, l, wo, scratch, temporal):
    for j in range(len(xs)):
        head_probs(scratch[0].at[j], scratch[1].at[j], scratch[2].at[j], temporal)
    for j in range(len(xs)):
        head_mix(values[j], scratch[2].at[j], scratch[3].at[j], temporal)
    return [(x + dot(scratch[3][j], wo[l], TN)).astype(BF16) for j, x in enumerate(xs)]


def attend(xs, l, norms, wq, wo, scratch, temporal):
    values = []
    for j, x in enumerate(xs):
        a = layer_norm(x, norms[l, 0:1, :], norms[l, 1:2, :])
        qT = dot(wq[l, 0:384, :], a, NT).astype(BF16)
        k = dot(a, wq[l, 384:768, :], NT).astype(BF16)
        values.append(dot(wq[l, 768:1152, :], a, NT).astype(BF16))
        head_scores(qT, k, scratch[0].at[j], temporal)
    return attend_end(xs, values, l, wo, scratch, temporal)


def mlp(res, l, norms, wu, wd, hid):
    res = res.astype(F32)
    half = layer_norm(res, 0.5 * norms[l, 2:3, :], 0.5 * norms[l, 3:4, :])
    for c in range(0, HIDDEN, 512):
        hid[:, c:c + 512] = gelu_of_half(dot(half, wu[l, :, c:c + 512], NN))
    return res + dot(hid[...], wd[l], NN)


def kernel(x_hbm, norms_hbm, wq_hbm, wo_hbm, wu_hbm, wd_hbm, y_hbm,
           xb, norms, wq, wo, wu, wd, hid, res, sent0, cols1, sent1, frames2, sent2, cols3, value_rows, queries, keys, values,
           load_sem, send_sem, recv_sem, *scratch):
    me = lax.axis_index('sp')
    pairs = ((wq_hbm, wq), (wo_hbm, wo), (wu_hbm, wu), (wd_hbm, wd))
    loads = [[pltpu.make_async_copy(s.at[l], d.at[l], load_sem.at[l, i]) for i, (s, d) in enumerate(pairs)]
             for l in range(4)]
    x_load = pltpu.make_async_copy(x_hbm, xb, load_sem.at[4, 0])
    norms_load = pltpu.make_async_copy(norms_hbm, norms, load_sem.at[4, 1])
    x_load.start()
    norms_load.start()
    for c in loads[0][:2]:
        c.start()
    barrier = pltpu.get_barrier_semaphore()
    for d in range(1, 4):
        pl.semaphore_signal(barrier, inc=1, device_id={'sp': (me + d) % 4}, device_id_type=MESH)

    def to_columns(e, src, dst, g, d):
        peer = (me + d) % 4
        return pltpu.make_async_remote_copy(
            src_ref=src.at[g, peer], dst_ref=dst.at[g, pl.ds(4 * me, 4)],
            send_sem=send_sem.at[e, g, d - 1], recv_sem=recv_sem.at[e, g, d - 1],
            device_id={'sp': peer}, device_id_type=MESH)

    def to_frames(e, src, dst, g, d):
        peer = (me + d) % 4
        return pltpu.make_async_remote_copy(
            src_ref=src.at[g, pl.ds(4 * peer, 4)], dst_ref=dst.at[me, g],
            send_sem=send_sem.at[e, g, d - 1], recv_sem=recv_sem.at[e, g, d - 1],
            device_id={'sp': peer}, device_id_type=MESH)

    def keep_queries(qk, at):
        queries[at] = qk[:, 0:384].astype(BF16).reshape(4, 4, 16, WIDTH)
        keys[at] = qk[:, 384:768].astype(BF16).reshape(4, 4, 16, WIDTH)

    def prepare_frames():
        for f in range(4):
            a = layer_norm(xb[f].reshape(256, WIDTH).astype(F32), norms[0, 0:1, :], norms[0, 1:2, :])
            keep_queries(dot(a, wq[0, 0:768, :], NT), (slice(None), slice(None), f))
            values[f] = dot(wq[0, 768:1152, :], a, NT).astype(BF16)

    def prepare_group(g, _):
        for d in (1, 2, 3):
            to_frames(1, sent1, frames2, g, d).wait_recv()
        x = frames2[:, g].reshape(256, WIDTH).astype(F32)
        a = layer_norm(x, norms[2, 0:1, :], norms[2, 1:2, :])
        qkv = dot(a, wq[2], NT)
        keep_queries(qkv, (slice(None), g))
        value_rows[:, g] = qkv[:, 768:1152].astype(BF16).reshape(4, 4, 16, WIDTH)
        return 0

    def prepare_values():
        for f in range(4):
            values[f] = value_rows[:, :, f].reshape(256, WIDTH).T

    def attend_half(l, half, read):
        scores, expd, probs, mixed = scratch
        groups = pl.ds(2 * half, 2)
        low = lax.broadcasted_iota(jnp.int32, (128, 128), 1) < 64
        for f in range(4):
            q = queries[:, groups, f].reshape(128, WIDTH)
            k = keys[:, :, f].reshape(256, WIDTH)
            for p in range(3):
                qp = q[:, 128 * p:128 * p + 128]
                zero = jnp.zeros_like(qp)
                rhs = jnp.concatenate([jnp.where(low, qp, zero), jnp.where(low, zero, qp)], 0)
                scores[f // 2, 3 * (f % 2) + p] = dot(k[:, 128 * p:128 * p + 128], rhs, NT)
        for j in range(2):
            head_probs(scores.at[j], expd.at[j], probs.at[j], False)
        for f in range(4):
            lanes = 128 * (f % 2)
            for p in range(3):
                r = 128 * p
                o = dot(values[f, r:r + 128, :], probs[f // 2, 3 * (f % 2) + p], NN).astype(BF16)
                mixed[f // 2, r:r + 64, lanes:lanes + 128] = o[0:64, 0:128]
                mixed[f // 2, r + 64:r + 128, lanes:lanes + 128] = o[64:128, 128:256]
        for j in range(2):
            x = jnp.concatenate([read(2 * j + u, groups).reshape(128, WIDTH) for u in range(2)], 0)
            rows = (x.astype(F32) + dot(mixed[j], wo[l], TN)).astype(BF16)
            for u in range(2):
                res[2 * j + u, :, groups] = rows[128 * u:128 * u + 128].reshape(4, 2, 16, WIDTH)

    def spatial_rest(l, e, read, sent, dst, before_send):
        def half_step(half, _):
            attend_half(l, half, read)
            def group_mlp(u):
                rows = jnp.stack([res[:, j, 2 * half + u] for j in range(4)])
                z = mlp(rows.reshape(256, WIDTH), l, norms, wu, wd, hid.at[u])
                sent[2 * half + u] = z.astype(BF16).reshape(4, 4, 16, WIDTH)

            def send(u):
                g = 2 * half + u
                for d in (2, 1, 3):
                    to_columns(e, sent, dst, g, d).start()
                dst[g, pl.ds(4 * me, 4)] = sent[g, me]

            if l in LATE:
                for u in range(2):
                    group_mlp(u)
                for u in range(2):
                    send(u)
            else:
                for u in range(2):
                    group_mlp(u)
                    send(u)
            return 0
        before_send()
        lax.fori_loop(0, 2, half_step, 0)

    def temporal(l, e, src, write):
        n = 2 if l in PAIRED else 1

        def body(i, _):
            xs = []
            for j in range(n):
                for d in (1, 2, 3):
                    to_columns(e, sent0, src, n * i + j, d).wait_recv()
            for j in range(n):
                xs.append(swap_halves(src[n * i + j].reshape(256, WIDTH).astype(F32), 16, 2))
            rows = attend(xs, l, norms, wq, wo, scratch, True)
            zs = [mlp(rows[j], l, norms, wu, wd, hid.at[j]) for j in range(n)]
            for j in range(n):
                write(n * i + j, swap_halves(zs[j], 2, 16).astype(BF16).reshape(16, 16, WIDTH))
            return 0
        lax.fori_loop(0, 4 // n, body, 0)

    def send_to_frames(g, z):
        sent1[g] = z
        for d in (2, 1, 3):
            to_frames(1, sent1, frames2, g, d).start()
        frames2[me, g] = sent1[g, pl.ds(4 * me, 4)]

    def write_y(g, z):
        y_hbm[:, pl.ds(pl.multiple_of(16 * g, 16), 16), :] = z

    def wait_weights(l):
        for c in loads[l]:
            c.wait()

    x_load.wait()
    norms_load.wait()
    for c in loads[0][:2]:
        c.wait()
    for c in loads[0][2:]:
        c.start()
    prepare_frames()

    def block0_ready():
        for c in loads[0][2:]:
            c.wait()
        for c in loads[1] + loads[2] + loads[3]:
            c.start()
        pl.semaphore_wait(barrier, 3)

    spatial_rest(0, 0, lambda f, groups: xb[f, :, groups], sent0, cols1, block0_ready)
    wait_weights(1)
    temporal(1, 0, cols1, send_to_frames)
    wait_weights(2)
    lax.fori_loop(0, 4, prepare_group, 0)
    prepare_values()
    spatial_rest(2, 2, lambda f, groups: frames2[:, groups, f], sent2, cols3, lambda: None)
    wait_weights(3)
    temporal(3, 2, cols3, write_y)
    for g in range(4):
        for d in (1, 2, 3):
            to_columns(0, sent0, cols1, g, d).wait_send()
            to_frames(1, sent1, frames2, g, d).wait_send()
            to_columns(2, sent2, cols3, g, d).wait_send()


def solution(mesh):
    anyspace = pl.BlockSpec(memory_space=pltpu.HBM)

    def local_stack(latents, norms, w_qkv, w_out, w_up, w_down):
        tokens = (4, 4, 4, 16, WIDTH)
        groups = (4, 16, 16, WIDTH)
        out = pl.pallas_call(
            kernel,
            out_shape=jax.ShapeDtypeStruct((16, 64, WIDTH), BF16),
            in_specs=[anyspace] * 6,
            out_specs=pl.BlockSpec(memory_space=pltpu.VMEM),
            scratch_shapes=[
                pltpu.VMEM(tokens, BF16), pltpu.VMEM((4, 4, WIDTH), F32),
                pltpu.VMEM((4, 1152, WIDTH), BF16), pltpu.VMEM((4, WIDTH, WIDTH), BF16),
                pltpu.VMEM((4, WIDTH, HIDDEN), BF16), pltpu.VMEM((4, HIDDEN, WIDTH), BF16),
                pltpu.VMEM((2, 256, HIDDEN), BF16),
                pltpu.VMEM(tokens, BF16),
                pltpu.VMEM(tokens, BF16), pltpu.VMEM(groups, BF16),
                pltpu.VMEM(groups, BF16), pltpu.VMEM(tokens, BF16),
                pltpu.VMEM(tokens, BF16), pltpu.VMEM(groups, BF16),
                pltpu.VMEM(tokens, BF16), pltpu.VMEM(tokens, BF16), pltpu.VMEM(tokens, BF16),
                pltpu.VMEM((4, WIDTH, 256), BF16),
                pltpu.SemaphoreType.DMA((6, 4)),
                pltpu.SemaphoreType.DMA((3, 4, 3)),
                pltpu.SemaphoreType.DMA((3, 4, 3)),
                pltpu.VMEM((2, 6, 256, 256), F32), pltpu.VMEM((2, 6, 256, 256), F32),
                pltpu.VMEM((2, 6, 256, 256), BF16), pltpu.VMEM((2, WIDTH, 256), BF16),
            ],
            compiler_params=pltpu.CompilerParams(collective_id=0, has_side_effects=True, vmem_limit_bytes=48 * 2**20),
        )(*[pltpu.with_memory_space_constraint(a, pltpu.HBM) for a in (
            latents.reshape(tokens), norms,
            w_qkv.transpose(0, 2, 3, 4, 1).reshape(4, 3 * WIDTH, WIDTH),
            w_out.reshape(4, WIDTH, WIDTH), w_up, w_down)])
        return out[None]

    whole = P()
    return jax.shard_map(local_stack, mesh=mesh,
                         in_specs=(P('data', 'sp', None, None), whole, whole, whole, whole, whole),
                         out_specs=P('data', None, 'sp', None), check_vma=False)
```

```python
import jax
import jax.numpy as jnp
from jax import lax
from jax.experimental import pallas as pl
from jax.experimental.pallas import tpu as pltpu
from jax.sharding import PartitionSpec as P

F32, BF16 = jnp.float32, jnp.bfloat16
EPS = 1e-6
WIDTH, HIDDEN = 384, 1536
NT = (((1,), (1,)), ((), ()))
NN = (((1,), (0,)), ((), ()))
TN = (((0,), (0,)), ((), ()))
SCORE_SCALE = 0.125 * 1.4426950408889634
MESH = pl.DeviceIdType.MESH
PAIRED, LATE = (3,), ()


def dot(a, b, dims):
    return lax.dot_general(a, b, dims, preferred_element_type=F32)


def layer_norm(x, gain, shift):
    centered = x - jnp.sum(x, -1, keepdims=True) * (1.0 / WIDTH)
    variance = jnp.sum(centered * centered, -1, keepdims=True) * (1.0 / WIDTH)
    return (centered * lax.rsqrt(variance + EPS) * gain + shift).astype(BF16)


def gelu_of_half(h):
    c = 0.7978845608028654
    return (h + h * jnp.tanh(h * (2.0 * c + (8.0 * c * 0.044715) * (h * h)))).astype(BF16)


def swap_halves(x, a, b):
    return x.reshape(a, b, 8, WIDTH).transpose(1, 0, 2, 3).reshape(256, WIDTH)


def head_scores(qT, k, scores, temporal):
    if not temporal:
        zero = jnp.zeros((64, 256), BF16)
        for h in range(6):
            qh = qT[64 * h:64 * h + 64, :]
            rhs = jnp.concatenate([zero, qh] if h % 2 else [qh, zero], 0)
            p = h // 2 * 128
            scores[h] = dot(k[:, p:p + 128], rhs, NN)
    else:
        zero = jnp.zeros((64, 128), BF16)
        row = lax.broadcasted_iota(jnp.int32, (128, 256), 0)
        col = lax.broadcasted_iota(jnp.int32, (128, 256), 1)
        same_patch = (row & 7) == (col & 7)
        for h in range(6):
            p, t = h // 2 * 128, h % 2 * 128
            q0 = jnp.concatenate([qT[p:p + 64, t:t + 128], zero], 1)
            q1 = jnp.concatenate([zero, qT[p + 64:p + 128, t:t + 128]], 1)
            s = dot(k[t:t + 128, p:p + 128], jnp.concatenate([q0, q1], 0), NN)
            scores[h, 0:128] = jnp.where(same_patch, s, -jnp.inf)


def head_probs(scores, expd, probs, temporal):
    keys = 128 if temporal else 256
    for h in range(6):
        peak = jnp.max(scores[h, 0:keys], 0, keepdims=True)
        e = jnp.exp2((scores[h, 0:keys] - peak) * SCORE_SCALE)
        expd[h, 0:keys] = e
        inverse = 1.0 / jnp.sum(e, 0, keepdims=True)
        probs[h, 0:keys] = (expd[h, 0:keys] * inverse).astype(BF16)


def head_mix(vT, probs, mixed, temporal):
    for h in range(6):
        if not temporal:
            r = 64 * h
            mixed[r:r + 64, :] = dot(vT[r:r + 64, :], probs[h], NN).astype(BF16)
        else:
            p, t = h // 2 * 128, h % 2 * 128
            o = dot(vT[p:p + 128, t:t + 128], probs[h, 0:128], NN).astype(BF16)
            mixed[p:p + 64, t:t + 128] = o[0:64, 0:128]
            mixed[p + 64:p + 128, t:t + 128] = o[64:128, 128:256]


def attend_end(xs, values, l, wo, scratch, temporal):
    for j in range(len(xs)):
        head_probs(scratch[0].at[j], scratch[1].at[j], scratch[2].at[j], temporal)
    for j in range(len(xs)):
        head_mix(values[j], scratch[2].at[j], scratch[3].at[j], temporal)
    return [(x + dot(scratch[3][j], wo[l], TN)).astype(BF16) for j, x in enumerate(xs)]


def attend(xs, l, norms, wq, wo, scratch, temporal):
    values = []
    for j, x in enumerate(xs):
        a = layer_norm(x, norms[l, 0:1, :], norms[l, 1:2, :])
        qT = dot(wq[l, 0:384, :], a, NT).astype(BF16)
        k = dot(a, wq[l, 384:768, :], NT).astype(BF16)
        values.append(dot(wq[l, 768:1152, :], a, NT).astype(BF16))
        head_scores(qT, k, scratch[0].at[j], temporal)
    return attend_end(xs, values, l, wo, scratch, temporal)


def mlp(res, l, norms, wu, wd, hid):
    res = res.astype(F32)
    half = layer_norm(res, 0.5 * norms[l, 2:3, :], 0.5 * norms[l, 3:4, :])
    for c in range(0, HIDDEN, 512):
        hid[:, c:c + 512] = gelu_of_half(dot(half, wu[l, :, c:c + 512], NN))
    return res + dot(hid[...], wd[l], NN)


def kernel(x_hbm, norms_hbm, wq_hbm, wo_hbm, wu_hbm, wd_hbm, y_hbm,
           xb, norms, wq, wo, wu, wd, hid, res, sent0, cols1, sent1, frames2, sent2, cols3, value_rows, queries, keys, values,
           load_sem, send_sem, recv_sem, *scratch):
    me = lax.axis_index('sp')
    pairs = ((wq_hbm, wq), (wo_hbm, wo), (wu_hbm, wu), (wd_hbm, wd))
    loads = [[pltpu.make_async_copy(s.at[l], d.at[l], load_sem.at[l, i]) for i, (s, d) in enumerate(pairs)]
             for l in range(4)]
    x_load = pltpu.make_async_copy(x_hbm, xb, load_sem.at[4, 0])
    norms_load = pltpu.make_async_copy(norms_hbm, norms, load_sem.at[4, 1])
    x_load.start()
    norms_load.start()
    loads[0][0].start()
    barrier = pltpu.get_barrier_semaphore()
    for d in range(1, 4):
        pl.semaphore_signal(barrier, inc=1, device_id={'sp': (me + d) % 4}, device_id_type=MESH)

    def to_columns(e, src, dst, g, d):
        peer = (me + d) % 4
        return pltpu.make_async_remote_copy(
            src_ref=src.at[g, peer], dst_ref=dst.at[g, pl.ds(4 * me, 4)],
            send_sem=send_sem.at[e, g, d - 1], recv_sem=recv_sem.at[e, g, d - 1],
            device_id={'sp': peer}, device_id_type=MESH)

    def to_frames(e, src, dst, g, d):
        peer = (me + d) % 4
        return pltpu.make_async_remote_copy(
            src_ref=src.at[g, pl.ds(4 * peer, 4)], dst_ref=dst.at[me, g],
            send_sem=send_sem.at[e, g, d - 1], recv_sem=recv_sem.at[e, g, d - 1],
            device_id={'sp': peer}, device_id_type=MESH)

    def keep_queries(qk, at):
        queries[at] = qk[:, 0:384].astype(BF16).reshape(4, 4, 16, WIDTH)
        keys[at] = qk[:, 384:768].astype(BF16).reshape(4, 4, 16, WIDTH)

    def prepare_frames():
        for f in range(4):
            a = layer_norm(xb[f].reshape(256, WIDTH).astype(F32), norms[0, 0:1, :], norms[0, 1:2, :])
            keep_queries(dot(a, wq[0, 0:768, :], NT), (slice(None), slice(None), f))
            values[f] = dot(wq[0, 768:1152, :], a, NT).astype(BF16)

    def prepare_group(g, _):
        for d in (1, 2, 3):
            to_frames(1, sent1, frames2, g, d).wait_recv()
        x = frames2[:, g].reshape(256, WIDTH).astype(F32)
        a = layer_norm(x, norms[2, 0:1, :], norms[2, 1:2, :])
        qkv = dot(a, wq[2], NT)
        keep_queries(qkv, (slice(None), g))
        value_rows[:, g] = qkv[:, 768:1152].astype(BF16).reshape(4, 4, 16, WIDTH)
        return 0

    def prepare_values():
        for f in range(4):
            values[f] = value_rows[:, :, f].reshape(256, WIDTH).T

    def attend_half(l, half, read):
        scores, expd, probs, mixed = scratch
        groups = pl.ds(2 * half, 2)
        low = lax.broadcasted_iota(jnp.int32, (128, 128), 1) < 64
        for f in range(4):
            q = queries[:, groups, f].reshape(128, WIDTH)
            k = keys[:, :, f].reshape(256, WIDTH)
            for p in range(3):
                qp = q[:, 128 * p:128 * p + 128]
                zero = jnp.zeros_like(qp)
                rhs = jnp.concatenate([jnp.where(low, qp, zero), jnp.where(low, zero, qp)], 0)
                scores[f // 2, 3 * (f % 2) + p] = dot(k[:, 128 * p:128 * p + 128], rhs, NT)
        for j in range(2):
            head_probs(scores.at[j], expd.at[j], probs.at[j], False)
        for f in range(4):
            lanes = 128 * (f % 2)
            for p in range(3):
                r = 128 * p
                o = dot(values[f, r:r + 128, :], probs[f // 2, 3 * (f % 2) + p], NN).astype(BF16)
                mixed[f // 2, r:r + 64, lanes:lanes + 128] = o[0:64, 0:128]
                mixed[f // 2, r + 64:r + 128, lanes:lanes + 128] = o[64:128, 128:256]
        for j in range(2):
            x = jnp.concatenate([read(2 * j + u, groups).reshape(128, WIDTH) for u in range(2)], 0)
            rows = (x.astype(F32) + dot(mixed[j], wo[l], TN)).astype(BF16)
            for u in range(2):
                res[2 * j + u, :, groups] = rows[128 * u:128 * u + 128].reshape(4, 2, 16, WIDTH)

    def spatial_rest(l, e, read, sent, dst, before_send):
        def half_step(half, _):
            attend_half(l, half, read)
            def group_mlp(u):
                rows = jnp.stack([res[:, j, 2 * half + u] for j in range(4)])
                z = mlp(rows.reshape(256, WIDTH), l, norms, wu, wd, hid.at[u])
                sent[2 * half + u] = z.astype(BF16).reshape(4, 4, 16, WIDTH)

            def send(u):
                g = 2 * half + u
                for d in (2, 1, 3):
                    to_columns(e, sent, dst, g, d).start()
                dst[g, pl.ds(4 * me, 4)] = sent[g, me]

            if l in LATE:
                for u in range(2):
                    group_mlp(u)
                for u in range(2):
                    send(u)
            else:
                for u in range(2):
                    group_mlp(u)
                    send(u)
            return 0
        before_send()
        lax.fori_loop(0, 2, half_step, 0)

    def temporal(l, e, src, write):
        n = 2 if l in PAIRED else 1

        def body(i, _):
            xs = []
            for j in range(n):
                for d in (1, 2, 3):
                    to_columns(e, sent0, src, n * i + j, d).wait_recv()
            for j in range(n):
                xs.append(swap_halves(src[n * i + j].reshape(256, WIDTH).astype(F32), 16, 2))
            rows = attend(xs, l, norms, wq, wo, scratch, True)
            zs = [mlp(rows[j], l, norms, wu, wd, hid.at[j]) for j in range(n)]
            for j in range(n):
                write(n * i + j, swap_halves(zs[j], 2, 16).astype(BF16).reshape(16, 16, WIDTH))
            return 0
        lax.fori_loop(0, 4 // n, body, 0)

    def send_to_frames(g, z):
        sent1[g] = z
        for d in (2, 1, 3):
            to_frames(1, sent1, frames2, g, d).start()
        frames2[me, g] = sent1[g, pl.ds(4 * me, 4)]

    def write_y(g, z):
        y_hbm[:, pl.ds(pl.multiple_of(16 * g, 16), 16), :] = z

    def wait_weights(l):
        for c in loads[l]:
            c.wait()

    x_load.wait()
    norms_load.wait()
    loads[0][0].wait()
    for c in loads[0][1:]:
        c.start()
    prepare_frames()

    def block0_ready():
        for c in loads[0][1:]:
            c.wait()
        for c in loads[1] + loads[2] + loads[3]:
            c.start()
        pl.semaphore_wait(barrier, 3)

    spatial_rest(0, 0, lambda f, groups: xb[f, :, groups], sent0, cols1, block0_ready)
    wait_weights(1)
    temporal(1, 0, cols1, send_to_frames)
    wait_weights(2)
    lax.fori_loop(0, 4, prepare_group, 0)
    prepare_values()
    spatial_rest(2, 2, lambda f, groups: frames2[:, groups, f], sent2, cols3, lambda: None)
    wait_weights(3)
    temporal(3, 2, cols3, write_y)
    for g in range(4):
        for d in (1, 2, 3):
            to_columns(0, sent0, cols1, g, d).wait_send()
            to_frames(1, sent1, frames2, g, d).wait_send()
            to_columns(2, sent2, cols3, g, d).wait_send()


def solution(mesh):
    anyspace = pl.BlockSpec(memory_space=pltpu.HBM)

    def local_stack(latents, norms, w_qkv, w_out, w_up, w_down):
        tokens = (4, 4, 4, 16, WIDTH)
        groups = (4, 16, 16, WIDTH)
        out = pl.pallas_call(
            kernel,
            out_shape=jax.ShapeDtypeStruct((16, 64, WIDTH), BF16),
            in_specs=[anyspace] * 6,
            out_specs=pl.BlockSpec(memory_space=pltpu.VMEM),
            scratch_shapes=[
                pltpu.VMEM(tokens, BF16), pltpu.VMEM((4, 4, WIDTH), F32),
                pltpu.VMEM((4, 1152, WIDTH), BF16), pltpu.VMEM((4, WIDTH, WIDTH), BF16),
                pltpu.VMEM((4, WIDTH, HIDDEN), BF16), pltpu.VMEM((4, HIDDEN, WIDTH), BF16),
                pltpu.VMEM((2, 256, HIDDEN), BF16),
                pltpu.VMEM(tokens, BF16),
                pltpu.VMEM(tokens, BF16), pltpu.VMEM(groups, BF16),
                pltpu.VMEM(groups, BF16), pltpu.VMEM(tokens, BF16),
                pltpu.VMEM(tokens, BF16), pltpu.VMEM(groups, BF16),
                pltpu.VMEM(tokens, BF16), pltpu.VMEM(tokens, BF16), pltpu.VMEM(tokens, BF16),
                pltpu.VMEM((4, WIDTH, 256), BF16),
                pltpu.SemaphoreType.DMA((6, 4)),
                pltpu.SemaphoreType.DMA((3, 4, 3)),
                pltpu.SemaphoreType.DMA((3, 4, 3)),
                pltpu.VMEM((2, 6, 256, 256), F32), pltpu.VMEM((2, 6, 256, 256), F32),
                pltpu.VMEM((2, 6, 256, 256), BF16), pltpu.VMEM((2, WIDTH, 256), BF16),
            ],
            compiler_params=pltpu.CompilerParams(collective_id=0, has_side_effects=True, vmem_limit_bytes=48 * 2**20),
        )(*[pltpu.with_memory_space_constraint(a, pltpu.HBM) for a in (
            latents.reshape(tokens), norms,
            w_qkv.transpose(0, 2, 3, 4, 1).reshape(4, 3 * WIDTH, WIDTH),
            w_out.reshape(4, WIDTH, WIDTH), w_up, w_down)])
        return out[None]

    whole = P()
    return jax.shard_map(local_stack, mesh=mesh,
                         in_specs=(P('data', 'sp', None, None), whole, whole, whole, whole, whole),
                         out_specs=P('data', None, 'sp', None), check_vma=False)
```
